32 devices in a mesh: dp: 16 (over z, x, core), mp: 2 (over y).
Axes of the slice: x: 2, y: 2, z: 4, core: 2. Of those that a mesh axis runs over, the one named last changes fastest.
Arguments:
- context: bfloat16 [5120, 2048], P('dp', 'mp'), may hold values from -6 to 6
- out_weight: bfloat16 [2048, 3584], P('mp'), may hold values from -0.125 to 0.125
- cotangent: bfloat16 [5120, 3584], P('dp'), may hold values from -0.059814453 to 0.059814453
- norm_gain: float32 [3584], replicated, may hold values from 0.5 to 1.5
- first_moment: float32 [2, 1024, 3584], P('mp', 'dp'), may hold values from -6 to 6
- second_moment: float32 [2, 1024, 3584], P('mp', 'dp'), may hold values from 0.01 to 1
Outputs:
- new_weight: bfloat16 [2, 1024, 3584], P('mp', 'dp')
- new_first: float32 [2, 1024, 3584], P('mp', 'dp')
- new_second: float32 [2, 1024, 3584], P('mp', 'dp')
- grad_gain: float32 [3584], replicated
- grad_context: bfloat16 [5120, 2048], P('dp', 'mp')
The draws below stay inside these ranges and needn't reach their ends.
All inputs are finite; a program needn't handle non-finite values.
Results may differ from the reference program's by a relative error of at most 0.005.
Values may be sent and summed in bfloat16 or wider, within the bound.
A program may use at most 128 MiB of HBM per device.

```python
import math
import jax
import jax.numpy as jnp
from jax import lax

D = 3584
HQ = 2048
TOKENS = 5120
N_MP = 2


def with_spikes(result, own_key, source, target, parts, factor):
    def block_of(position):
        return (jnp.arange(result.shape[position]) // (result.shape[position] // parts)).reshape((-1,) + (1,) * (result.ndim - 1 - position))

    one_side = jax.random.permutation(own_key, parts)[block_of(target)]
    second = (block_of(target) + parts // 2) % parts
    return jnp.where((block_of(source) == one_side) | (block_of(source) == second), factor * result, result)


def shard_levels(stream_key, extent, split, least, high):
    gain, own = 1.0, jax.random.fold_in(stream_key, 6)
    for position, blocks in split:
        steps = jnp.exp(jax.random.uniform(jax.random.fold_in(own, position), (blocks,), jnp.float32, least / len(split), high / len(split)))
        gain = gain * jnp.repeat(steps, extent[position] // blocks).reshape([-1 if axis == position else 1 for axis in range(len(extent))])
    return gain


def centred(key, extent, spread, reach, pieces=(), dtype=jnp.bfloat16):
    gain = shard_levels(key, extent, pieces, -0.22, 0.18) if pieces else 1.0
    entries = jax.random.normal(key, extent, jnp.float32) * spread * gain
    return jnp.minimum(jnp.maximum(entries, -reach), reach).astype(dtype)


def gaussian_with(own_key, shape, width, limit, cuts, heavy, held_as=jnp.bfloat16):
    array = width * jax.random.normal(own_key, shape, jnp.float32)
    if cuts:
        array = array * shard_levels(own_key, shape, cuts, -0.22, 0.18)
    return jnp.clip(with_spikes(array, jax.random.fold_in(own_key, 3), *heavy), -limit, limit).astype(held_as)


def setup_inputs(seed: int = 0) -> dict:
    arg_keys = jax.random.split(jax.random.key(seed), 7)
    return {
        "context": gaussian_with(arg_keys[0], (TOKENS, HQ), 1.0, 6.0, ((0, 16), (1, 2)), (0, 1, 16, 2.0)),
        "out_weight": centred(arg_keys[1], (HQ, D), HQ ** -0.5, 0.125, ((0, 2),)),
        "cotangent": centred(arg_keys[2], (TOKENS, D), 0.01, 0.059814453, ((0, 16),)),
        "norm_gain": jnp.clip(1.0 + 0.1 * jax.random.normal(arg_keys[3], (D,), jnp.float32), 0.5, 1.5),
        "first_moment": centred(arg_keys[4], (N_MP, HQ // N_MP, D), 1.0, 6.0, ((0, 2), (1, 16)), jnp.float32),
        "second_moment": jnp.clip(jnp.exp(math.log(1.0) - 4.6051702 * jax.random.uniform(arg_keys[5], (N_MP, HQ // N_MP, D), jnp.float32) ** shard_levels(arg_keys[5], (N_MP, HQ // N_MP, D), ((0, 2), (1, 16)), -0.2, 0.2)), 0.01, 1.0),
    }


norm_floor = 0.1
learn_rate = 0.01
beta_one = 0.9
beta_two = 0.95
adam_floor = 1e-08

def reference(context, out_weight, cotangent, norm_gain, first_moment, second_moment):
    attn = jnp.dot(context, out_weight, preferred_element_type=jnp.float32)
    inverse = lax.rsqrt(lax.optimization_barrier(jnp.mean(attn * attn, axis=-1, keepdims=True)) + norm_floor)
    normed = attn * inverse
    upstream = cotangent.astype(jnp.float32)
    scaled = upstream * norm_gain
    grad_gain = lax.optimization_barrier(jnp.sum(upstream * normed, axis=0))
    grad_attn = (inverse * (scaled - normed * lax.optimization_barrier(jnp.mean(scaled * normed, axis=-1, keepdims=True)))).astype(jnp.bfloat16)
    grad_context = jnp.dot(grad_attn, out_weight.T, preferred_element_type=jnp.float32).astype(jnp.bfloat16)
    grad_weight = jnp.dot(context.T, grad_attn, preferred_element_type=jnp.float32)
    grad_weight = grad_weight.reshape(N_MP, HQ // N_MP, D)
    new_first = beta_one * first_moment + (1.0 - beta_one) * grad_weight
    new_second = beta_two * second_moment + (1.0 - beta_two) * grad_weight * grad_weight
    master = out_weight.astype(jnp.float32).reshape(N_MP, HQ // N_MP, D)
    new_weight = (master - learn_rate * new_first / (jnp.sqrt(new_second) + adam_floor)).astype(jnp.bfloat16)
    return (new_weight, new_first, new_second, grad_gain, grad_context)
```

```python
import functools

import jax
import jax.numpy as jnp
from jax import lax
from jax.experimental import pallas as pl
from jax.experimental.pallas import tpu as pltpu
from jax.sharding import PartitionSpec as P

norm_floor = 0.1
learn_rate = 0.01
beta_one = 0.9
beta_two = 0.95
adam_floor = 1e-08

MESH = pl.DeviceIdType.MESH
F32 = jnp.float32
BF16 = jnp.bfloat16
VMEM_LIMIT = 50 * 1024 * 1024
LAG = 2
PRE = 5


def kernel(
    cfg,
    ctx_hbm, w_hbm, cot_hbm, gain_hbm, m1_hbm, m2_hbm,
    nw, n1, n2, gfin, gc_out,
    wv, ctx, ctxt_all, ctxt, cot, gain_flat, gain, psend, precv, own, stat_s, stat_r, g4, gx,
    sends, recvs, keeps, fsend, frecv, m1, m2, master, gc_acc,
    gp, gpr,
    in_sem, w_sem, cot_sem, m_sem,
    ps_s, ps_r, st_s, st_r, cx_s, cx_r, gy_s, gy_r, gx_s, gx_r, gm_s, gm_r, gr_s, gr_r,
    rs_s, rs_r, fx_s, fx_r, gg_s, gg_r,
):
    n, bits, quarter, cw, rows, tok, heads, width = cfg
    half = 2 * quarter
    chunks = 4 * quarter
    stages = bits - 2
    dp, mp = lax.axis_index("dp"), lax.axis_index("mp")
    peer = 1 - mp
    side = (dp // 2) % 2
    order = [*range(2, bits), 1]

    def flip(index, bit):
        return index + (1 << bit) * (1 - 2 * ((index // (1 << bit)) % 2))

    def peer_id():
        return (dp, peer)

    def bit_id(bit):
        return (flip(dp, bit), mp)

    def place(r):
        group = r // quarter
        across = group // 2
        x_side = side + across * (1 - 2 * side)
        y_half = mp + (group % 2) * (1 - 2 * mp)
        return (2 * y_half + x_side) * quarter + r % quarter

    def column(r):
        return pl.multiple_of(place(r) * cw, cw)

    def mine(h):
        return h + quarter * (h // quarter)

    def ctx_copy():
        return pltpu.make_async_copy(ctx_hbm, ctx.at[pl.ds(0, tok)], in_sem.at[0])

    def gain_copy():
        return pltpu.make_async_copy(gain_hbm, gain_flat, in_sem.at[1])

    def w_copy(r):
        return pltpu.make_async_copy(w_hbm.at[:, pl.ds(column(r), cw)], wv.at[r], w_sem.at[r])

    def cot_copy(h):
        return pltpu.make_async_copy(cot_hbm.at[:, pl.ds(column(mine(h)), cw)], cot.at[h], cot_sem.at[h])

    def m_copies():
        return (
            pltpu.make_async_copy(m1_hbm.at[0], m1, m_sem.at[0]),
            pltpu.make_async_copy(m2_hbm.at[0], m2, m_sem.at[1]),
            pltpu.make_async_copy(
                w_hbm.at[pl.ds(pl.multiple_of(dp * rows, rows), rows), :], master, m_sem.at[2]
            ),
        )

    def remote(src, dst, send_sem, recv_sem, device):
        return pltpu.make_async_remote_copy(
            src_ref=src, dst_ref=dst, send_sem=send_sem, recv_sem=recv_sem,
            device_id=device, device_id_type=MESH,
        )

    def partial_send(h):
        return remote(psend.at[h], precv.at[h], ps_s.at[h], ps_r.at[h], peer_id())

    def stat_send():
        return remote(stat_s, stat_r, st_s, st_r, peer_id())

    def ctx_send(a, b, i, bit):
        return remote(
            ctx.at[pl.ds(a * tok, tok)], ctx.at[pl.ds(b * tok, tok)], cx_s.at[i], cx_r.at[i], bit_id(bit)
        )

    def ctx_mate():
        return ctx_send(0, 1, 0, 0)

    def ctx_side():
        return ctx_send(0, 2, 1, 1)

    def ctx_relay():
        return ctx_send(2, 3, 2, 0)

    def grad_peer_near(j):
        return remote(
            g4.at[j, pl.ds(0, tok)], g4.at[quarter + j, pl.ds(0, tok)],
            gy_s.at[j], gy_r.at[j], peer_id(),
        )

    def grad_peer_far(j):
        return remote(
            gx.at[j], gx.at[quarter + j], gy_s.at[quarter + j], gy_r.at[quarter + j], peer_id()
        )

    def grad_side(i):
        return remote(gx.at[i], g4.at[i, pl.ds(2 * tok, tok)], gx_s.at[i], gx_r.at[i], bit_id(1))

    def grad_mate(i):
        return remote(
            g4.at[i, pl.ds(0, tok)], g4.at[i, pl.ds(tok, tok)], gm_s.at[i], gm_r.at[i], bit_id(0)
        )

    def grad_relay(i):
        return remote(
            g4.at[i, pl.ds(2 * tok, tok)], g4.at[i, pl.ds(3 * tok, tok)],
            gr_s.at[i], gr_r.at[i], bit_id(0),
        )

    def shard_send(s, i):
        return remote(
            sends[s].at[i], recvs[s].at[i], rs_s.at[s, i], rs_r.at[s, i], bit_id(order[s])
        )

    def swap_send(i):
        return remote(fsend.at[i], frecv.at[i], fx_s.at[i], fx_r.at[i], bit_id(1))

    steps = [0, *order]

    def gain_send(b):
        device = bit_id(steps[b]) if b < bits else peer_id()
        return remote(gp.at[b], gpr.at[b], gg_s.at[b], gg_r.at[b], device)

    ctx_copy().start()

    @pl.loop(0, quarter)
    def _(j):
        w_copy(quarter + j).start()
        w_copy(3 * quarter + j).start()

    barrier = pltpu.get_barrier_semaphore()
    pl.semaphore_signal(barrier, inc=1, device_id=peer_id(), device_id_type=MESH)
    for bit in range(bits):
        pl.semaphore_signal(barrier, inc=1, device_id=bit_id(bit), device_id_type=MESH)

    gain_copy().start()

    @pl.loop(0, quarter)
    def _(j):
        w_copy(j).start()
        w_copy(2 * quarter + j).start()
        cot_copy(j).start()
        cot_copy(quarter + j).start()

    for copy in m_copies():
        copy.start()

    def pair(near, far):
        w_copy(near).wait()
        w_copy(far).wait()
        return jnp.dot(
            ctx[0:tok], jnp.concatenate([wv[near], wv[far]], axis=1), preferred_element_type=F32
        )

    def partial(j):
        value = pair(quarter + j, 3 * quarter + j).astype(BF16)
        psend[j] = value[:, :cw]
        psend[quarter + j] = value[:, cw:]

    def partial_start(j):
        partial_send(j).start()
        partial_send(quarter + j).start()

    ctx_copy().wait()
    partial(0)
    pl.semaphore_wait(barrier, bits + 1)
    partial_start(0)
    ctx_side().start()
    ctx_mate().start()

    @pl.loop(1, quarter)
    def _(j):
        partial(j)
        partial_start(j)

    @pl.loop(0, quarter)
    def _(j):
        value = pair(j, 2 * quarter + j)
        own[j] = value[:, :cw]
        own[quarter + j] = value[:, cw:]

    gain_copy().wait()
    for r in range(chunks):
        gain[r] = gain_flat[r * cw:(r + 1) * cw].reshape(1, cw)

    def turn(p):
        ctxt_all[...] = jnp.transpose(
            ctx[2 * p * tok:2 * (p + 1) * tok].astype(F32)
        ).reshape(n, rows, 2 * tok)
        blocks = []
        for spot in range(n // 2):
            shard = dp
            for i, k in enumerate(order):
                if not (spot >> (bits - 2 - i)) & 1:
                    shard = flip(shard, k)
            blocks.append(ctxt_all[shard])
        ctxt[p] = jnp.concatenate(blocks, axis=0).astype(BF16)

    ctx_mate().wait_recv()
    turn(0)

    def gather_stats(h, carry):
        square, cross = carry
        cot_copy(h).wait()
        partial_send(h).wait_recv()
        attn = own[h] + precv[h].astype(F32)
        own[h] = attn
        scaled = cot[h].astype(F32) * gain[place(mine(h))]
        return square + attn * attn, cross + scaled * attn

    def gather_pair(j, carry):
        return gather_stats(quarter + j, gather_stats(j, carry))

    early, late = (2 * quarter) // 3, (5 * quarter) // 6
    zero = jnp.zeros((tok, cw), F32)
    carry = lax.fori_loop(0, early, gather_pair, (zero, zero))
    ctx_side().wait_recv()
    ctx_relay().start()
    carry = lax.fori_loop(early, late, gather_pair, carry)
    ctx_relay().wait_recv()
    turn(1)
    square, cross = lax.fori_loop(late, quarter, gather_pair, carry)
    square = jnp.sum(square, axis=1, keepdims=True)
    cross = jnp.sum(cross, axis=1, keepdims=True)
    even = lax.broadcasted_iota(jnp.int32, (tok, 128), 1) % 2 == 0
    stat_s[...] = jnp.transpose(jnp.where(even, square, cross))[0:8]
    stat_send().start()
    stat_send().wait_recv()
    totals = jnp.transpose(jnp.concatenate([stat_s[...] + stat_r[...]] * 16, axis=0))
    inverse = lax.rsqrt(totals[:, 0:1] / width + norm_floor)
    shift = inverse * totals[:, 1:2] / width

    def gradient(h):
        spot = place(mine(h))
        upstream = cot[h].astype(F32)
        normed = own[h] * inverse
        gp[0, spot - half * mp] = jnp.sum(upstream * normed, axis=0, keepdims=True)
        return (inverse * (upstream * gain[spot] - normed * shift)).astype(BF16)

    @pl.loop(0, quarter)
    def _(j):
        gx[j] = gradient(quarter + j)
        grad_side(j).start()
        grad_peer_far(j).start()
        g4[j, 0:tok] = gradient(j)
        grad_mate(j).start()

    @pl.loop(0, quarter)
    def _(j):
        grad_peer_near(j).start()

    gain_send(0).start()

    def context_part(u):
        left = jnp.concatenate([g4[u, 0:tok], gx[u]], axis=1)
        right = jnp.concatenate([wv[u], wv[half + u]], axis=1)
        return lax.dot_general(left, right, (((1,), (1,)), ((), ())), preferred_element_type=F32)

    gc_acc[...] = context_part(0)

    @pl.loop(1, PRE)
    def _(u):
        gc_acc[...] += context_part(u)

    def adam(total, r):
        cols = pl.ds(column(r), cw)
        first = beta_one * m1[:, cols] + (1.0 - beta_one) * total
        second = beta_two * m2[:, cols] + (1.0 - beta_two) * total * total
        nw[0, :, cols] = (
            master[:, cols].astype(F32) - learn_rate * first / (jnp.sqrt(second) + adam_floor)
        ).astype(BF16)
        n1[0, :, cols] = first
        n2[0, :, cols] = second

    for copy in m_copies():
        copy.wait()

    n_final = half + LAG * (stages + 1)

    @pl.loop(0, max(n_final, 3 * bits + 3))
    def _(t):
        @pl.when(t < quarter)
        def _():
            grad_peer_far(t).wait_recv()
            grad_side(quarter + t).start()

        @pl.when((t >= quarter) & (t < half))
        def _():
            grad_peer_near(t - quarter).wait_recv()
            grad_mate(t).start()

        @pl.when(t < half)
        def _():
            grad_side(t).wait_recv()
            grad_relay(t).start()

        unit = jnp.where(t < quarter, t + PRE, t)

        @pl.when((t < half) & ((t >= quarter) | (unit < quarter)))
        def _():
            gc_acc[...] += context_part(unit)

        @pl.when(t == half)
        def _():
            gc_out[...] = gc_acc[...].astype(BF16)

        for b in range(bits + 1):
            @pl.when(t == 3 * b + 1)
            def _():
                gain_send(b).wait_recv()
                if b < bits:
                    gp[b + 1] = gp[b] + gpr[b]
                    gain_send(b + 1).start()
                else:
                    gfin[pl.ds(mp * half, half)] = gp[bits]
                    gfin[pl.ds(peer * half, half)] = gpr[bits]

        late_swap = t - LAG * (stages + 1)

        @pl.when((late_swap >= 0) & (late_swap < half))
        def _():
            swap_send(late_swap).wait_recv()
            adam(frecv[late_swap].astype(F32), half + late_swap)

        for s in range(stages - 1, -1, -1):
            i = t - LAG * (s + 1)

            @pl.when((i >= 0) & (i < half))
            def _():
                shard_send(s, i).wait_recv()
                total = keeps[s][i] + recvs[s][i].astype(F32)
                cut = total.shape[0] // 2
                if s < stages - 1:
                    sends[s + 1][i] = total[:cut].astype(BF16)
                    shard_send(s + 1, i).start()
                    keeps[s + 1][i] = total[cut:]
                else:
                    fsend[i] = total[:cut].astype(BF16)
                    swap_send(i).start()
                    adam(total[cut:], i)

        @pl.when(t < half)
        def _():
            grad_mate(t).wait_recv()
            grad_relay(t).wait_recv()
            product = jnp.dot(ctxt[0], g4[t, 0:2 * tok], preferred_element_type=F32)
            product += jnp.dot(ctxt[1], g4[t, 2 * tok:4 * tok], preferred_element_type=F32)
            cut = product.shape[0] // 2
            sends[0][t] = product[:cut].astype(BF16)
            shard_send(0, t).start()
            keeps[0][t] = product[cut:]

    stat_send().wait_send()
    ctx_mate().wait_send()
    ctx_side().wait_send()
    ctx_relay().wait_send()

    @pl.loop(0, quarter)
    def _(j):
        grad_peer_near(j).wait_send()
        grad_peer_far(j).wait_send()

    for b in range(bits + 1):
        gain_send(b).wait_send()

    @pl.loop(0, half)
    def _(i):
        partial_send(i).wait_send()
        grad_side(i).wait_send()
        grad_mate(i).wait_send()
        grad_relay(i).wait_send()
        swap_send(i).wait_send()
        for s in range(stages):
            shard_send(s, i).wait_send()


def settle(nw, n1, n2, gg, gc, nw_out, n1_out, n2_out, gg_out, gc_out, flat, sem):
    pairs = ((nw, nw_out), (n1, n1_out), (n2, n2_out), (gc, gc_out))
    copies = [pltpu.make_async_copy(a, b, sem.at[i]) for i, (a, b) in enumerate(pairs)]
    for copy in copies:
        copy.start()
    chunks, _, cw = gg.shape
    for r in range(chunks):
        flat[r * cw:(r + 1) * cw] = gg[r].reshape(cw)
    copies.append(pltpu.make_async_copy(flat, gg_out, sem.at[4]))
    copies[-1].start()
    for copy in copies:
        copy.wait()


def per_device(n, context, out_weight, cotangent, norm_gain, first_moment, second_moment):
    tok, heads = context.shape
    width = out_weight.shape[1]
    rows = first_moment.shape[1]
    bits = n.bit_length() - 1
    cw = 128
    quarter = width // (4 * cw)
    half, chunks = 2 * quarter, 4 * quarter
    stages = bits - 2
    cfg = (n, bits, quarter, cw, rows, tok, heads, width)
    sizes = [(n >> (s + 2)) * rows for s in range(stages)]
    dma = pltpu.SemaphoreType.DMA
    vmem = pltpu.VMEM
    scratch = [
        vmem((chunks, heads, cw), BF16),
        vmem((4 * tok, heads), BF16),
        vmem((n, rows, 2 * tok), F32),
        vmem((2, heads // 2, 2 * tok), BF16),
        vmem((half, tok, cw), BF16),
        vmem((width,), F32),
        vmem((chunks, 1, cw), F32),
        vmem((half, tok, cw), BF16),
        vmem((half, tok, cw), BF16),
        vmem((half, tok, cw), F32),
        vmem((8, tok), F32),
        vmem((8, tok), F32),
        vmem((half, 4 * tok, cw), BF16),
        vmem((half, tok, cw), BF16),
        tuple(vmem((half, size, cw), BF16) for size in sizes),
        tuple(vmem((half, size, cw), BF16) for size in sizes),
        tuple(vmem((half, size, cw), F32) for size in sizes),
        vmem((half, rows, cw), BF16),
        vmem((half, rows, cw), BF16),
        vmem((rows, width), F32),
        vmem((rows, width), F32),
        vmem((rows, width), BF16),
        vmem((tok, heads), F32),
        vmem((bits + 1, half, 1, cw), F32),
        vmem((bits + 1, half, 1, cw), F32),
        dma((2,)), dma((chunks,)), dma((half,)), dma((3,)),
        dma((half,)), dma((half,)), dma, dma, dma((3,)), dma((3,)),
        dma((half,)), dma((half,)), dma((half,)), dma((half,)),
        dma((half,)), dma((half,)), dma((half,)), dma((half,)),
        dma((stages, half)), dma((stages, half)), dma((half,)), dma((half,)),
        dma((bits + 1,)), dma((bits + 1,)),
    ]
    anywhere = pl.BlockSpec(memory_space=pltpu.HBM)
    new_weight, new_first, new_second, grad_gain, grad_context = pl.pallas_call(
        functools.partial(kernel, cfg),
        out_shape=(
            jax.ShapeDtypeStruct(first_moment.shape, BF16),
            jax.ShapeDtypeStruct(first_moment.shape, F32),
            jax.ShapeDtypeStruct(first_moment.shape, F32),
            jax.ShapeDtypeStruct((chunks, 1, cw), F32),
            jax.ShapeDtypeStruct((tok, heads), BF16),
        ),
        in_specs=[anywhere] * 6,
        out_specs=(pl.BlockSpec(memory_space=pltpu.VMEM),) * 5,
        scratch_shapes=scratch,
        compiler_params=pltpu.CompilerParams(
            collective_id=0, has_side_effects=True, vmem_limit_bytes=VMEM_LIMIT
        ),
    )(context, out_weight, cotangent, norm_gain, first_moment, second_moment)
    return pl.pallas_call(
        settle,
        out_shape=(
            jax.ShapeDtypeStruct(first_moment.shape, BF16),
            jax.ShapeDtypeStruct(first_moment.shape, F32),
            jax.ShapeDtypeStruct(first_moment.shape, F32),
            jax.ShapeDtypeStruct((width,), F32),
            jax.ShapeDtypeStruct((tok, heads), BF16),
        ),
        in_specs=[pl.BlockSpec(memory_space=pltpu.VMEM)] * 5,
        out_specs=(anywhere,) * 5,
        scratch_shapes=[vmem((width,), F32), dma((5,))],
        compiler_params=pltpu.CompilerParams(vmem_limit_bytes=8 * 1024 * 1024),
    )(new_weight, new_first, new_second, grad_gain, grad_context)


def solution(mesh):
    return jax.shard_map(
        functools.partial(per_device, mesh.shape["dp"]),
        mesh=mesh,
        in_specs=(
            P("dp", "mp"),
            P("mp", None),
            P("dp", None),
            P(),
            P("mp", "dp", None),
            P("mp", "dp", None),
        ),
        out_specs=(
            P("mp", "dp", None),
            P("mp", "dp", None),
            P("mp", "dp", None),
            P(),
            P("dp", "mp"),
        ),
        check_vma=False,
    )
```

```python
import functools

import jax
import jax.numpy as jnp
from jax import lax
from jax.experimental import pallas as pl
from jax.experimental.pallas import tpu as pltpu
from jax.sharding import PartitionSpec as P

norm_floor = 0.1
learn_rate = 0.01
beta_one = 0.9
beta_two = 0.95
adam_floor = 1e-08

MESH = pl.DeviceIdType.MESH
F32 = jnp.float32
BF16 = jnp.bfloat16
VMEM_LIMIT = 50 * 1024 * 1024
LAG = 2
SWAP = 8


def kernel(
    cfg,
    ctx_hbm, w_hbm, cot_hbm, gain_hbm, m1_hbm, m2_hbm,
    nw, n1, n2, gfin, gc_out,
    wv, ctx, ctxt_all, ctxt, cot, gain_flat, gain, psend, precv, own, stat_s, stat_r, inverse_v, shift_v, g4, gx,
    sends, recvs, keeps, fsend, frecv, m1, m2, master, gc_acc,
    gp, gpr,
    in_sem, w_sem, cot_sem, m_sem,
    ps_s, ps_r, st_s, st_r, cx_s, cx_r, gy_s, gy_r, gx_s, gx_r, gm_s, gm_r, gr_s, gr_r,
    rs_s, rs_r, fx_s, fx_r, gg_s, gg_r,
):
    n, bits, quarter, cw, rows, tok, heads, width = cfg
    half = 2 * quarter
    chunks = 4 * quarter
    stages = bits - 2
    dp, mp = lax.axis_index("dp"), lax.axis_index("mp")
    peer = 1 - mp
    side = (dp // 2) % 2
    order = [*range(2, bits), 1]

    def flip(index, bit):
        return index + (1 << bit) * (1 - 2 * ((index // (1 << bit)) % 2))

    def peer_id():
        return (dp, peer)

    def bit_id(bit):
        return (flip(dp, bit), mp)

    starts = [
        (2 * y_half + x_side) * quarter
        for x_side in (side, 1 - side) for y_half in (mp, peer)
    ]

    def cols(group, j):
        return pl.ds(pl.multiple_of((starts[group] + j) * cw, cw), cw)

    def cols_of(across, i):
        near, far = starts[2 * across:2 * across + 2]
        first = jnp.where(i < quarter, near + i, far + i - quarter)
        return pl.ds(pl.multiple_of(first * cw, cw), cw)

    def ctx_copy():
        return pltpu.make_async_copy(ctx_hbm, ctx.at[pl.ds(0, tok)], in_sem.at[0])

    def gain_copy():
        return pltpu.make_async_copy(gain_hbm, gain_flat, in_sem.at[1])

    def w_copy(group, j):
        r = group * quarter + j
        return pltpu.make_async_copy(w_hbm.at[:, cols(group, j)], wv.at[r], w_sem.at[r])

    def cot_copy(far, j):
        h = far * quarter + j
        return pltpu.make_async_copy(cot_hbm.at[:, cols(2 * far, j)], cot.at[h], cot_sem.at[h])

    def m_copies():
        return (
            pltpu.make_async_copy(m1_hbm.at[0], m1, m_sem.at[0]),
            pltpu.make_async_copy(m2_hbm.at[0], m2, m_sem.at[1]),
            pltpu.make_async_copy(
                w_hbm.at[pl.ds(pl.multiple_of(dp * rows, rows), rows), :], master, m_sem.at[2]
            ),
        )

    def remote(src, dst, send_sem, recv_sem, device):
        return pltpu.make_async_remote_copy(
            src_ref=src, dst_ref=dst, send_sem=send_sem, recv_sem=recv_sem,
            device_id=device, device_id_type=MESH,
        )

    def partial_send(h):
        return remote(psend.at[h], precv.at[h], ps_s.at[h], ps_r.at[h], peer_id())

    def stat_send():
        return remote(stat_s, stat_r, st_s, st_r, peer_id())

    def ctx_send(a, b, i, bit):
        return remote(
            ctx.at[pl.ds(a * tok, tok)], ctx.at[pl.ds(b * tok, tok)], cx_s.at[i], cx_r.at[i], bit_id(bit)
        )

    def ctx_mate():
        return ctx_send(0, 1, 0, 0)

    def ctx_side():
        return ctx_send(0, 2, 1, 1)

    def ctx_relay():
        return ctx_send(2, 3, 2, 0)

    def grad_peer_near(j):
        return remote(
            g4.at[j, pl.ds(0, tok)], g4.at[quarter + j, pl.ds(0, tok)],
            gy_s.at[j], gy_r.at[j], peer_id(),
        )

    def grad_peer_far(j):
        return remote(
            gx.at[j], gx.at[quarter + j], gy_s.at[quarter + j], gy_r.at[quarter + j], peer_id()
        )

    def grad_side(i):
        return remote(gx.at[i], g4.at[i, pl.ds(2 * tok, tok)], gx_s.at[i], gx_r.at[i], bit_id(1))

    def grad_mate(i):
        return remote(
            g4.at[i, pl.ds(0, tok)], g4.at[i, pl.ds(tok, tok)], gm_s.at[i], gm_r.at[i], bit_id(0)
        )

    def grad_relay(i):
        return remote(
            g4.at[i, pl.ds(2 * tok, tok)], g4.at[i, pl.ds(3 * tok, tok)],
            gr_s.at[i], gr_r.at[i], bit_id(0),
        )

    def shard_send(s, i):
        return remote(
            sends[s].at[i], recvs[s].at[i], rs_s.at[s, i], rs_r.at[s, i], bit_id(order[s])
        )

    def swap_send(i):
        return remote(fsend.at[i], frecv.at[i], fx_s.at[i], fx_r.at[i], bit_id(1))

    steps = [0, *order]

    def gain_send(b):
        device = bit_id(steps[b]) if b < bits else peer_id()
        return remote(gp.at[b], gpr.at[b], gg_s.at[b], gg_r.at[b], device)

    barrier = pltpu.get_barrier_semaphore()
    pl.semaphore_signal(barrier, inc=1, device_id=peer_id(), device_id_type=MESH)
    for bit in range(bits - 1, -1, -1):
        pl.semaphore_signal(barrier, inc=1, device_id=bit_id(bit), device_id_type=MESH)

    ctx_copy().start()

    @pl.loop(0, quarter)
    def _(j):
        w_copy(1, j).start()
        w_copy(3, j).start()

    def pair(near, far, j):
        w_copy(near, j).wait()
        w_copy(far, j).wait()
        right = jnp.concatenate([wv[near * quarter + j], wv[far * quarter + j]], axis=1)
        return jnp.dot(ctx[0:tok], right, preferred_element_type=F32)

    def partial(j):
        value = pair(1, 3, j).astype(BF16)
        psend[j] = value[:, :cw]
        psend[quarter + j] = value[:, cw:]

    def partial_start(j):
        partial_send(j).start()
        partial_send(quarter + j).start()

    ctx_copy().wait()
    partial(0)
    pl.semaphore_wait(barrier, bits + 1)
    partial_start(0)
    ctx_side().start()
    ctx_mate().start()

    @pl.loop(1, quarter)
    def _(j):
        partial(j)
        partial_start(j)
        w_copy(0, j).start()
        w_copy(2, j).start()
        cot_copy(0, j).start()
        cot_copy(1, j).start()

    for group in (0, 2):
        w_copy(group, 0).start()
        cot_copy(group // 2, 0).start()
    gain_copy().start()

    @pl.loop(1, quarter + 1)
    def _(k):
        j = jnp.where(k == quarter, 0, k)
        value = pair(0, 2, j)
        own[j] = value[:, :cw]
        own[quarter + j] = value[:, cw:]

    for copy in m_copies():
        copy.start()

    gain_copy().wait()
    for r in range(chunks):
        gain[r] = gain_flat[r * cw:(r + 1) * cw].reshape(1, cw)

    def turn(p):
        ctxt_all[...] = jnp.transpose(
            ctx[2 * p * tok:2 * (p + 1) * tok].astype(F32)
        ).reshape(n, rows, 2 * tok)
        blocks = []
        for spot in range(n // 2):
            shard = dp
            for i, k in enumerate(order):
                if not (spot >> (bits - 2 - i)) & 1:
                    shard = flip(shard, k)
            blocks.append(ctxt_all[shard])
        ctxt[p] = jnp.concatenate(blocks, axis=0).astype(BF16)

    ctx_mate().wait_recv()
    turn(0)

    def gather_stats(far, j, carry):
        square, cross = carry
        h = far * quarter + j
        cot_copy(far, j).wait()
        partial_send(h).wait_recv()
        attn = own[h] + precv[h].astype(F32)
        own[h] = attn
        scaled = cot[h].astype(F32) * gain[starts[2 * far] + j]
        return square + attn * attn, cross + scaled * attn

    def gather_pair(j, carry):
        return gather_stats(1, j, gather_stats(0, j, carry))

    early, late = (2 * quarter) // 3, (5 * quarter) // 6
    zero = jnp.zeros((tok, cw), F32)
    carry = lax.fori_loop(0, early, gather_pair, (zero, zero))
    ctx_side().wait_recv()
    ctx_relay().start()
    carry = lax.fori_loop(early, late, gather_pair, carry)
    ctx_relay().wait_recv()
    turn(1)
    square, cross = lax.fori_loop(late, quarter, gather_pair, carry)
    square = jnp.sum(square, axis=1, keepdims=True)
    cross = jnp.sum(cross, axis=1, keepdims=True)
    even = lax.broadcasted_iota(jnp.int32, (tok, 128), 1) % 2 == 0
    stat_s[...] = jnp.transpose(jnp.where(even, square, cross))[0:8]
    stat_send().start()
    stat_send().wait_recv()
    totals = stat_s[...] + stat_r[...]

    def spread(row):
        return jnp.transpose(jnp.concatenate([totals[row:row + 1]] * 128, axis=0))

    inverse = lax.rsqrt(spread(0) / width + norm_floor)
    inverse_v[...] = inverse
    shift_v[...] = inverse * spread(1) / width

    def gradient(far, j):
        h = far * quarter + j
        spot = starts[2 * far] + j
        inverse = inverse_v[...]
        upstream = cot[h].astype(F32)
        normed = own[h] * inverse
        gp[0, spot - half * mp] = jnp.sum(upstream * normed, axis=0, keepdims=True)
        return (inverse * (upstream * gain[spot] - normed * shift_v[...])).astype(BF16)

    @pl.loop(0, quarter)
    def _(j):
        gx[j] = gradient(1, j)
        grad_side(j).start()
        grad_peer_far(j).start()

    @pl.loop(0, quarter)
    def _(j):
        g4[j, 0:tok] = gradient(0, j)
        grad_mate(j).start()
        grad_peer_near(j).start()

    gain_send(0).start()

    def context_part(u):
        left = jnp.concatenate([g4[u, 0:tok], gx[u]], axis=1)
        right = jnp.concatenate([wv[u], wv[half + u]], axis=1)
        return lax.dot_general(left, right, (((1,), (1,)), ((), ())), preferred_element_type=F32)

    gc_acc[...] = context_part(0)

    @pl.loop(1, quarter)
    def _(u):
        gc_acc[...] += context_part(u)

    def adam(total, cols):
        first = beta_one * m1[:, cols] + (1.0 - beta_one) * total
        second = beta_two * m2[:, cols] + (1.0 - beta_two) * total * total
        nw[0, :, cols] = (
            master[:, cols].astype(F32) - learn_rate * first / (jnp.sqrt(second) + adam_floor)
        ).astype(BF16)
        n1[0, :, cols] = first
        n2[0, :, cols] = second

    for copy in m_copies():
        copy.wait()

    swap_lag = LAG * stages + SWAP

    @pl.loop(0, max(half + swap_lag, 3 * bits + 3))
    def _(t):
        @pl.when(t < half)
        def _():
            grad_side(t).wait_recv()
            grad_relay(t).start()

        @pl.when((t >= quarter) & (t < half))
        def _():
            grad_peer_near(t - quarter).wait_recv()
            grad_mate(t).start()
            gc_acc[...] += context_part(t)

        @pl.when(t == half)
        def _():
            gc_out[...] = gc_acc[...].astype(BF16)

        for b in range(bits + 1):
            @pl.when(t == 3 * b + 1)
            def _():
                gain_send(b).wait_recv()
                if b < bits:
                    gp[b + 1] = gp[b] + gpr[b]
                    gain_send(b + 1).start()
                else:
                    gfin[pl.ds(mp * half, half)] = gp[bits]
                    gfin[pl.ds(peer * half, half)] = gpr[bits]

        late_swap = t - swap_lag

        @pl.when((late_swap >= 0) & (late_swap < half))
        def _():
            swap_send(late_swap).wait_recv()
            adam(frecv[late_swap].astype(F32), cols_of(1, late_swap))

        for s in range(stages - 1, -1, -1):
            i = t - LAG * (s + 1)

            @pl.when((i >= 0) & (i < half))
            def _():
                shard_send(s, i).wait_recv()
                total = keeps[s][i] + recvs[s][i].astype(F32)
                cut = total.shape[0] // 2
                if s < stages - 1:
                    sends[s + 1][i] = total[:cut].astype(BF16)
                    shard_send(s + 1, i).start()
                    keeps[s + 1][i] = total[cut:]
                else:
                    fsend[i] = total[:cut].astype(BF16)
                    swap_send(i).start()
                    adam(total[cut:], cols_of(0, i))

        @pl.when(t < half)
        def _():
            grad_mate(t).wait_recv()
            grad_relay(t).wait_recv()
            product = jnp.dot(ctxt[0], g4[t, 0:2 * tok], preferred_element_type=F32)
            product += jnp.dot(ctxt[1], g4[t, 2 * tok:4 * tok], preferred_element_type=F32)
            cut = product.shape[0] // 2
            sends[0][t] = product[:cut].astype(BF16)
            shard_send(0, t).start()
            keeps[0][t] = product[cut:]

        @pl.when(t < quarter)
        def _():
            grad_peer_far(t).wait_recv()
            grad_side(quarter + t).start()

    stat_send().wait_send()
    ctx_mate().wait_send()
    ctx_side().wait_send()
    ctx_relay().wait_send()

    @pl.loop(0, quarter)
    def _(j):
        grad_peer_near(j).wait_send()
        grad_peer_far(j).wait_send()

    for b in range(bits + 1):
        gain_send(b).wait_send()

    @pl.loop(0, half)
    def _(i):
        partial_send(i).wait_send()
        grad_side(i).wait_send()
        grad_mate(i).wait_send()
        grad_relay(i).wait_send()
        swap_send(i).wait_send()
        for s in range(stages):
            shard_send(s, i).wait_send()


def settle(nw, n1, n2, gg, gc, nw_out, n1_out, n2_out, gg_out, gc_out, flat, sem):
    pairs = ((nw, nw_out), (n1, n1_out), (n2, n2_out), (gc, gc_out))
    copies = [pltpu.make_async_copy(a, b, sem.at[i]) for i, (a, b) in enumerate(pairs)]
    for copy in copies:
        copy.start()
    chunks, _, cw = gg.shape
    for r in range(chunks):
        flat[r * cw:(r + 1) * cw] = gg[r].reshape(cw)
    copies.append(pltpu.make_async_copy(flat, gg_out, sem.at[4]))
    copies[-1].start()
    for copy in copies:
        copy.wait()


def per_device(n, context, out_weight, cotangent, norm_gain, first_moment, second_moment):
    tok, heads = context.shape
    width = out_weight.shape[1]
    rows = first_moment.shape[1]
    bits = n.bit_length() - 1
    cw = 128
    quarter = width // (4 * cw)
    half, chunks = 2 * quarter, 4 * quarter
    stages = bits - 2
    cfg = (n, bits, quarter, cw, rows, tok, heads, width)
    sizes = [(n >> (s + 2)) * rows for s in range(stages)]
    dma = pltpu.SemaphoreType.DMA
    vmem = pltpu.VMEM
    scratch = [
        vmem((chunks, heads, cw), BF16),
        vmem((4 * tok, heads), BF16),
        vmem((n, rows, 2 * tok), F32),
        vmem((2, heads // 2, 2 * tok), BF16),
        vmem((half, tok, cw), BF16),
        vmem((width,), F32),
        vmem((chunks, 1, cw), F32),
        vmem((half, tok, cw), BF16),
        vmem((half, tok, cw), BF16),
        vmem((half, tok, cw), F32),
        vmem((8, tok), F32),
        vmem((8, tok), F32),
        vmem((tok, cw), F32),
        vmem((tok, cw), F32),
        vmem((half, 4 * tok, cw), BF16),
        vmem((half, tok, cw), BF16),
        tuple(vmem((half, size, cw), BF16) for size in sizes),
        tuple(vmem((half, size, cw), BF16) for size in sizes),
        tuple(vmem((half, size, cw), F32) for size in sizes),
        vmem((half, rows, cw), BF16),
        vmem((half, rows, cw), BF16),
        vmem((rows, width), F32),
        vmem((rows, width), F32),
        vmem((rows, width), BF16),
        vmem((tok, heads), F32),
        vmem((bits + 1, half, 1, cw), F32),
        vmem((bits + 1, half, 1, cw), F32),
        dma((2,)), dma((chunks,)), dma((half,)), dma((3,)),
        dma((half,)), dma((half,)), dma, dma, dma((3,)), dma((3,)),
        dma((half,)), dma((half,)), dma((half,)), dma((half,)),
        dma((half,)), dma((half,)), dma((half,)), dma((half,)),
        dma((stages, half)), dma((stages, half)), dma((half,)), dma((half,)),
        dma((bits + 1,)), dma((bits + 1,)),
    ]
    anywhere = pl.BlockSpec(memory_space=pltpu.HBM)
    pin = functools.partial(pltpu.with_memory_space_constraint, memory_space=pltpu.HBM)
    new_weight, new_first, new_second, grad_gain, grad_context = pl.pallas_call(
        functools.partial(kernel, cfg),
        out_shape=(
            jax.ShapeDtypeStruct(first_moment.shape, BF16),
            jax.ShapeDtypeStruct(first_moment.shape, F32),
            jax.ShapeDtypeStruct(first_moment.shape, F32),
            jax.ShapeDtypeStruct((chunks, 1, cw), F32),
            jax.ShapeDtypeStruct((tok, heads), BF16),
        ),
        in_specs=[anywhere] * 6,
        out_specs=(pl.BlockSpec(memory_space=pltpu.VMEM),) * 5,
        scratch_shapes=scratch,
        compiler_params=pltpu.CompilerParams(
            collective_id=0, has_side_effects=True, vmem_limit_bytes=VMEM_LIMIT
        ),
    )(*map(pin, (context, out_weight, cotangent, norm_gain, first_moment, second_moment)))
    return pl.pallas_call(
        settle,
        out_shape=(
            jax.ShapeDtypeStruct(first_moment.shape, BF16),
            jax.ShapeDtypeStruct(first_moment.shape, F32),
            jax.ShapeDtypeStruct(first_moment.shape, F32),
            jax.ShapeDtypeStruct((width,), F32),
            jax.ShapeDtypeStruct((tok, heads), BF16),
        ),
        in_specs=[pl.BlockSpec(memory_space=pltpu.VMEM)] * 5,
        out_specs=(anywhere,) * 5,
        scratch_shapes=[vmem((width,), F32), dma((5,))],
        compiler_params=pltpu.CompilerParams(vmem_limit_bytes=8 * 1024 * 1024),
    )(new_weight, new_first, new_second, grad_gain, grad_context)


def solution(mesh):
    return jax.shard_map(
        functools.partial(per_device, mesh.shape["dp"]),
        mesh=mesh,
        in_specs=(
            P("dp", "mp"),
            P("mp", None),
            P("dp", None),
            P(),
            P("mp", "dp", None),
            P("mp", "dp", None),
        ),
        out_specs=(
            P("mp", "dp", None),
            P("mp", "dp", None),
            P("mp", "dp", None),
            P(),
            P("dp", "mp"),
        ),
        check_vma=False,
    )
```

```python
import functools

import jax
import jax.numpy as jnp
from jax import lax
from jax.experimental import pallas as pl
from jax.experimental.pallas import tpu as pltpu
from jax.sharding import PartitionSpec as P

norm_floor = 0.1
learn_rate = 0.01
beta_one = 0.9
beta_two = 0.95
adam_floor = 1e-08

MESH = pl.DeviceIdType.MESH
F32 = jnp.float32
BF16 = jnp.bfloat16
VMEM_LIMIT = 50 * 1024 * 1024
LAG = 3
SWAP = 6
FIRST = 2


def kernel(
    cfg,
    ctx_hbm, w_hbm, cot_hbm, gain_hbm, m1_hbm, m2_hbm,
    nw, n1, n2, gfin, gc_out,
    wv, ctx, ctxt_all, ctxt, cot, gain_flat, gain, psend, precv, own, stat_s, stat_r, inverse_v, shift_v, g4, gx,
    sends, recvs, keeps, fsend, frecv, m1, m2, master, gc_acc,
    gp, gpr,
    in_sem, w_sem, cot_sem, m_sem,
    ps_s, ps_r, st_s, st_r, cx_s, cx_r, gy_s, gy_r, gx_s, gx_r, gm_s, gm_r,
    rs_s, rs_r, fx_s, fx_r, gg_s, gg_r,
):
    n, bits, quarter, cw, rows, tok, heads, width = cfg
    half = 2 * quarter
    chunks = 4 * quarter
    stages = bits - 2
    dp, mp = lax.axis_index("dp"), lax.axis_index("mp")
    peer = 1 - mp
    side = (dp // 2) % 2
    order = [*range(2, bits), 1]

    def flip(index, bit):
        return index + (1 << bit) * (1 - 2 * ((index // (1 << bit)) % 2))

    def peer_id():
        return (dp, peer)

    def bit_id(bit):
        return (flip(dp, bit), mp)

    starts = [
        (2 * y_half + x_side) * quarter
        for x_side in (side, 1 - side) for y_half in (mp, peer)
    ]

    def cols(group, j):
        return pl.ds(pl.multiple_of((starts[group] + j) * cw, cw), cw)

    def cols_of(across, i):
        near, far = starts[2 * across:2 * across + 2]
        first = jnp.where(i < quarter, near + i, far + i - quarter)
        return pl.ds(pl.multiple_of(first * cw, cw), cw)

    def ctx_copy():
        return pltpu.make_async_copy(ctx_hbm, ctx.at[pl.ds(0, tok)], in_sem.at[0])

    def gain_copy():
        return pltpu.make_async_copy(gain_hbm, gain_flat, in_sem.at[1])

    def w_copy(group, j, sem):
        base = half * (1 - group % 2)
        return pltpu.make_async_copy(
            w_hbm.at[:, cols(group, j)], wv.at[base + 2 * j + group // 2], sem
        )

    def w_wait(first, last, sem):
        block = wv.at[pl.ds(first, last - first)]
        pltpu.make_async_copy(block, block, sem).wait()

    def cot_copy(far, j):
        h = far * quarter + j
        return pltpu.make_async_copy(cot_hbm.at[:, cols(2 * far, j)], cot.at[h], cot_sem)

    def m_copies():
        return (
            pltpu.make_async_copy(m1_hbm.at[0], m1, m_sem.at[0]),
            pltpu.make_async_copy(m2_hbm.at[0], m2, m_sem.at[1]),
            pltpu.make_async_copy(
                w_hbm.at[pl.ds(pl.multiple_of(dp * rows, rows), rows), :], master, m_sem.at[2]
            ),
        )

    def remote(src, dst, send_sem, recv_sem, device):
        return pltpu.make_async_remote_copy(
            src_ref=src, dst_ref=dst, send_sem=send_sem, recv_sem=recv_sem,
            device_id=device, device_id_type=MESH,
        )

    def partial_send(h):
        return remote(psend.at[h], precv.at[h], ps_s, ps_r.at[h], peer_id())

    def stat_send():
        return remote(stat_s, stat_r, st_s, st_r, peer_id())

    def ctx_send(a, b, i, bit):
        return remote(
            ctx.at[pl.ds(a * tok, tok)], ctx.at[pl.ds(b * tok, tok)], cx_s, cx_r.at[i], bit_id(bit)
        )

    def ctx_mate():
        return ctx_send(0, 1, 0, 0)

    def ctx_side():
        return ctx_send(0, 2, 1, 1)

    def ctx_relay():
        return ctx_send(2, 3, 2, 0)

    def grad_peer_near(j):
        return remote(
            g4.at[j, pl.ds(0, tok)], g4.at[quarter + j, pl.ds(0, tok)],
            gy_s.at[0], gy_r.at[j], peer_id(),
        )

    def grad_peer_far(j):
        return remote(
            gx.at[j], gx.at[quarter + j], gy_s.at[1], gy_r.at[quarter + j], peer_id()
        )

    def grad_side(i):
        return remote(gx.at[i], g4.at[i, pl.ds(2 * tok, tok)], gx_s, gx_r.at[i], bit_id(1))

    def grad_mate(i):
        return remote(
            g4.at[i, pl.ds(0, tok)], g4.at[i, pl.ds(tok, tok)], gm_s.at[0], gm_r.at[i], bit_id(0)
        )

    def grad_relay(i):
        return remote(
            g4.at[i, pl.ds(2 * tok, tok)], g4.at[i, pl.ds(3 * tok, tok)],
            gm_s.at[1], gm_r.at[i], bit_id(0),
        )

    def grad_chip(i):
        both = g4.at[i, pl.ds(0, 2 * tok)]
        return remote(both, both, gm_s.at[0], gm_r.at[i], bit_id(0))

    def shard_send(s, i):
        return remote(
            sends[s].at[i], recvs[s].at[i], rs_s.at[s], rs_r.at[s, i], bit_id(order[s])
        )

    def swap_send(i):
        return remote(fsend.at[i], frecv.at[i], fx_s, fx_r.at[i], bit_id(1))

    steps = [0, *order]

    def gain_send(b):
        device = bit_id(steps[b]) if b < bits else peer_id()
        return remote(gp.at[b], gpr.at[b], gg_s, gg_r.at[b], device)

    barrier = pltpu.get_barrier_semaphore()
    pl.semaphore_signal(barrier, inc=1, device_id=peer_id(), device_id_type=MESH)
    for bit in range(bits - 1, -1, -1):
        pl.semaphore_signal(barrier, inc=1, device_id=bit_id(bit), device_id_type=MESH)

    ctx_copy().start()
    w_copy(1, 0, w_sem.at[0]).start()
    w_copy(3, 0, w_sem.at[0]).start()

    def pair(base, j):
        right = jnp.concatenate([wv[base + 2 * j], wv[base + 2 * j + 1]], axis=1)
        return jnp.dot(ctx[0:tok], right, preferred_element_type=F32)

    def partial(j):
        value = pair(0, j).astype(BF16)
        psend[j] = value[:, :cw]
        psend[quarter + j] = value[:, cw:]

    def partial_start(j):
        partial_send(j).start()
        partial_send(quarter + j).start()

    ctx_copy().wait()
    w_wait(0, 2, w_sem.at[0])

    @pl.loop(1, quarter)
    def _(j):
        w_copy(1, j, w_sem.at[1]).start()
        w_copy(3, j, w_sem.at[1]).start()

    @pl.loop(0, quarter)
    def _(j):
        w_copy(0, j, w_sem.at[2]).start()
        w_copy(2, j, w_sem.at[2]).start()

    partial(0)
    pl.semaphore_wait(barrier, bits + 1)

    partial_start(0)
    w_wait(2, half, w_sem.at[1])

    @pl.loop(1, quarter)
    def _(j):
        partial(j)
        partial_start(j)
        cot_copy(0, j).start()
        cot_copy(1, j).start()

    ctx_side().start()
    ctx_mate().start()
    cot_copy(0, 0).start()
    cot_copy(1, 0).start()
    gain_copy().start()
    w_wait(half, chunks, w_sem.at[2])

    @pl.loop(0, quarter)
    def _(j):
        value = pair(half, j)
        own[j] = value[:, :cw]
        own[quarter + j] = value[:, cw:]

    for copy in m_copies():
        copy.start()

    gain_copy().wait()
    for r in range(chunks):
        gain[r] = gain_flat[r * cw:(r + 1) * cw].reshape(1, cw)

    def turn(p):
        ctxt_all[...] = jnp.transpose(
            ctx[2 * p * tok:2 * (p + 1) * tok].astype(F32)
        ).reshape(n, rows, 2 * tok)
        blocks = []
        for spot in range(n // 2):
            shard = dp
            for i, k in enumerate(order):
                if not (spot >> (bits - 2 - i)) & 1:
                    shard = flip(shard, k)
            blocks.append(ctxt_all[shard])
        ctxt[p] = jnp.concatenate(blocks, axis=0).astype(BF16)

    pltpu.make_async_copy(cot, cot, cot_sem).wait()
    ctx_mate().wait_recv()
    turn(0)

    def gather_stats(far, j, carry):
        square, cross = carry
        h = far * quarter + j
        partial_send(h).wait_recv()
        attn = own[h] + precv[h].astype(F32)
        own[h] = attn
        scaled = cot[h].astype(F32) * gain[starts[2 * far] + j]
        return square + attn * attn, cross + scaled * attn

    def gather_pair(j, carry):
        return gather_stats(1, j, gather_stats(0, j, carry))

    early, late = (2 * quarter) // 3, (5 * quarter) // 6
    zero = jnp.zeros((tok, cw), F32)
    carry = lax.fori_loop(0, early, gather_pair, (zero, zero))
    ctx_side().wait_recv()
    ctx_relay().start()
    carry = lax.fori_loop(early, late, gather_pair, carry)
    ctx_relay().wait_recv()
    turn(1)
    square, cross = lax.fori_loop(late, quarter, gather_pair, carry)
    square = jnp.sum(square, axis=1, keepdims=True)
    cross = jnp.sum(cross, axis=1, keepdims=True)
    even = lax.broadcasted_iota(jnp.int32, (tok, 128), 1) % 2 == 0
    stat_s[...] = jnp.transpose(jnp.where(even, square, cross))[0:8]
    stat_send().start()
    stat_send().wait_recv()
    totals = stat_s[...] + stat_r[...]

    def spread(row):
        return jnp.transpose(jnp.concatenate([totals[row:row + 1]] * 128, axis=0))

    inverse = lax.rsqrt(spread(0) / width + norm_floor)
    inverse_v[...] = inverse
    shift_v[...] = inverse * spread(1) / width

    def gradient(far, j):
        h = far * quarter + j
        spot = starts[2 * far] + j
        inverse = inverse_v[...]
        upstream = cot[h].astype(F32)
        normed = own[h] * inverse
        gp[0, spot - half * mp] = jnp.sum(upstream * normed, axis=0, keepdims=True)
        return (inverse * (upstream * gain[spot] - normed * shift_v[...])).astype(BF16)

    def far_part(j):
        gx[j] = gradient(1, j)
        grad_side(j).start()
        grad_peer_far(j).start()

    @pl.loop(0, FIRST)
    def _(j):
        far_part(j)

    @pl.loop(0, quarter)
    def _(j):
        g4[j, 0:tok] = gradient(0, j)
        grad_mate(j).start()

    def context_part(u, base):
        left = jnp.concatenate([g4[u, 0:tok], gx[u]], axis=1)
        right = jnp.concatenate([wv[base], wv[base + 1]], axis=1)
        return lax.dot_general(left, right, (((1,), (1,)), ((), ())), preferred_element_type=F32)

    gc_acc[...] = context_part(0, half)

    @pl.loop(FIRST, quarter)
    def _(j):
        far_part(j)

    gain_send(0).start()

    @pl.loop(0, quarter)
    def _(j):
        grad_peer_near(j).start()

    @pl.loop(1, quarter)
    def _(u):
        gc_acc[...] += context_part(u, half + 2 * u)

    def adam(total, cols):
        first = beta_one * m1[:, cols] + (1.0 - beta_one) * total
        second = beta_two * m2[:, cols] + (1.0 - beta_two) * total * total
        nw[0, :, cols] = (
            master[:, cols].astype(F32) - learn_rate * first / (jnp.sqrt(second) + adam_floor)
        ).astype(BF16)
        n1[0, :, cols] = first
        n2[0, :, cols] = second

    for copy in m_copies():
        copy.wait()

    swap_lag = LAG * stages + SWAP

    @pl.loop(0, max(half + swap_lag, 3 * bits + 3))
    def _(t):
        @pl.when(t < half)
        def _():
            grad_side(t).wait_recv()
            grad_relay(t).start()

        @pl.when((t >= quarter) & (t < half))
        def _():
            grad_peer_near(t - quarter).wait_recv()
            grad_mate(t).start()
            gc_acc[...] += context_part(t, 2 * (t - quarter))

        @pl.when(t == half)
        def _():
            gc_out[...] = gc_acc[...].astype(BF16)

        for b in range(bits + 1):
            @pl.when(t == 3 * b + 1)
            def _():
                gain_send(b).wait_recv()
                if b < bits:
                    gp[b + 1] = gp[b] + gpr[b]
                    gain_send(b + 1).start()
                else:
                    gfin[pl.ds(mp * half, half)] = gp[bits]
                    gfin[pl.ds(peer * half, half)] = gpr[bits]

        late_swap = t - swap_lag

        @pl.when((late_swap >= 0) & (late_swap < half))
        def _():
            swap_send(late_swap).wait_recv()
            adam(frecv[late_swap].astype(F32), cols_of(1, late_swap))

        for s in range(stages - 1, -1, -1):
            i = t - LAG * (s + 1)

            @pl.when((i >= 0) & (i < half))
            def _():
                shard_send(s, i).wait_recv()
                total = keeps[s][i] + recvs[s][i].astype(F32)
                cut = total.shape[0] // 2
                if s < stages - 1:
                    sends[s + 1][i] = total[:cut].astype(BF16)
                    shard_send(s + 1, i).start()
                    keeps[s + 1][i] = total[cut:]
                else:
                    fsend[i] = total[:cut].astype(BF16)
                    swap_send(i).start()
                    adam(total[cut:], cols_of(0, i))

        @pl.when(t < half)
        def _():
            grad_chip(t).wait_recv()
            product = jnp.dot(ctxt[0], g4[t, 0:2 * tok], preferred_element_type=F32)
            product += jnp.dot(ctxt[1], g4[t, 2 * tok:4 * tok], preferred_element_type=F32)
            cut = product.shape[0] // 2
            sends[0][t] = product[:cut].astype(BF16)
            shard_send(0, t).start()
            keeps[0][t] = product[cut:]

        @pl.when(t < quarter)
        def _():
            grad_peer_far(t).wait_recv()
            grad_side(quarter + t).start()

    def drain(block, sem):
        remote(block, block, sem, st_r, peer_id()).wait_send()

    stat_send().wait_send()
    drain(ctx.at[pl.ds(0, 3 * tok)], cx_s)
    drain(psend, ps_s)
    drain(gx.at[pl.ds(0, quarter)], gy_s.at[0])
    drain(gx.at[pl.ds(0, quarter)], gy_s.at[1])
    drain(gx, gx_s)
    drain(gx, gm_s.at[0])
    drain(gx, gm_s.at[1])
    drain(gp, gg_s)
    drain(fsend, fx_s)
    for s in range(stages):
        drain(sends[s], rs_s.at[s])


def settle(nw, n1, n2, gg, gc, nw_out, n1_out, n2_out, gg_out, gc_out, flat, sem):
    pairs = ((nw, nw_out), (n1, n1_out), (n2, n2_out), (gc, gc_out))
    copies = [pltpu.make_async_copy(a, b, sem.at[i]) for i, (a, b) in enumerate(pairs)]
    for copy in copies:
        copy.start()
    chunks, _, cw = gg.shape
    for r in range(chunks):
        flat[r * cw:(r + 1) * cw] = gg[r].reshape(cw)
    copies.append(pltpu.make_async_copy(flat, gg_out, sem.at[4]))
    copies[-1].start()
    for copy in copies:
        copy.wait()


def per_device(n, context, out_weight, cotangent, norm_gain, first_moment, second_moment):
    tok, heads = context.shape
    width = out_weight.shape[1]
    rows = first_moment.shape[1]
    bits = n.bit_length() - 1
    cw = 128
    quarter = width // (4 * cw)
    half, chunks = 2 * quarter, 4 * quarter
    stages = bits - 2
    cfg = (n, bits, quarter, cw, rows, tok, heads, width)
    sizes = [(n >> (s + 2)) * rows for s in range(stages)]
    dma = pltpu.SemaphoreType.DMA
    vmem = pltpu.VMEM
    scratch = [
        vmem((chunks, heads, cw), BF16),
        vmem((4 * tok, heads), BF16),
        vmem((n, rows, 2 * tok), F32),
        vmem((2, heads // 2, 2 * tok), BF16),
        vmem((half, tok, cw), BF16),
        vmem((width,), F32),
        vmem((chunks, 1, cw), F32),
        vmem((half, tok, cw), BF16),
        vmem((half, tok, cw), BF16),
        vmem((half, tok, cw), F32),
        vmem((8, tok), F32),
        vmem((8, tok), F32),
        vmem((tok, cw), F32),
        vmem((tok, cw), F32),
        vmem((half, 4 * tok, cw), BF16),
        vmem((half, tok, cw), BF16),
        tuple(vmem((half, size, cw), BF16) for size in sizes),
        tuple(vmem((half, size, cw), BF16) for size in sizes),
        tuple(vmem((half, size, cw), F32) for size in sizes),
        vmem((half, rows, cw), BF16),
        vmem((half, rows, cw), BF16),
        vmem((rows, width), F32),
        vmem((rows, width), F32),
        vmem((rows, width), BF16),
        vmem((tok, heads), F32),
        vmem((bits + 1, half, 1, cw), F32),
        vmem((bits + 1, half, 1, cw), F32),
        dma((2,)), dma((3,)), dma, dma((3,)),
        dma, dma((half,)), dma, dma, dma, dma((3,)),
        dma((2,)), dma((half,)), dma, dma((half,)), dma((2,)), dma((half,)),
        dma((stages,)), dma((stages, half)), dma, dma((half,)),
        dma, dma((bits + 1,)),
    ]
    anywhere = pl.BlockSpec(memory_space=pltpu.HBM)
    pin = functools.partial(pltpu.with_memory_space_constraint, memory_space=pltpu.HBM)
    new_weight, new_first, new_second, grad_gain, grad_context = pl.pallas_call(
        functools.partial(kernel, cfg),
        out_shape=(
            jax.ShapeDtypeStruct(first_moment.shape, BF16),
            jax.ShapeDtypeStruct(first_moment.shape, F32),
            jax.ShapeDtypeStruct(first_moment.shape, F32),
            jax.ShapeDtypeStruct((chunks, 1, cw), F32),
            jax.ShapeDtypeStruct((tok, heads), BF16),
        ),
        in_specs=[anywhere] * 6,
        out_specs=(pl.BlockSpec(memory_space=pltpu.VMEM),) * 5,
        scratch_shapes=scratch,
        compiler_params=pltpu.CompilerParams(
            collective_id=0, has_side_effects=True, vmem_limit_bytes=VMEM_LIMIT
        ),
    )(*map(pin, (context, out_weight, cotangent, norm_gain, first_moment, second_moment)))
    return pl.pallas_call(
        settle,
        out_shape=(
            jax.ShapeDtypeStruct(first_moment.shape, BF16),
            jax.ShapeDtypeStruct(first_moment.shape, F32),
            jax.ShapeDtypeStruct(first_moment.shape, F32),
            jax.ShapeDtypeStruct((width,), F32),
            jax.ShapeDtypeStruct((tok, heads), BF16),
        ),
        in_specs=[pl.BlockSpec(memory_space=pltpu.VMEM)] * 5,
        out_specs=(anywhere,) * 5,
        scratch_shapes=[vmem((width,), F32), dma((5,))],
        compiler_params=pltpu.CompilerParams(vmem_limit_bytes=8 * 1024 * 1024),
    )(new_weight, new_first, new_second, grad_gain, grad_context)


def solution(mesh):
    return jax.shard_map(
        functools.partial(per_device, mesh.shape["dp"]),
        mesh=mesh,
        in_specs=(
            P("dp", "mp"),
            P("mp", None),
            P("dp", None),
            P(),
            P("mp", "dp", None),
            P("mp", "dp", None),
        ),
        out_specs=(
            P("mp", "dp", None),
            P("mp", "dp", None),
            P("mp", "dp", None),
            P(),
            P("dp", "mp"),
        ),
        check_vma=False,
    )
```

```python
import functools

import jax
import jax.numpy as jnp
from jax import lax
from jax.experimental import pallas as pl
from jax.experimental.pallas import tpu as pltpu
from jax.sharding import PartitionSpec as P

norm_floor = 0.1
learn_rate = 0.01
beta_one = 0.9
beta_two = 0.95
adam_floor = 1e-08

MESH = pl.DeviceIdType.MESH
F32 = jnp.float32
BF16 = jnp.bfloat16
VMEM_LIMIT = 50 * 1024 * 1024
LAG = 3
SWAP = 6
FIRST = 2
WARM = 3


def kernel(
    cfg,
    ctx_hbm, w_hbm, cot_hbm, gain_hbm, m1_hbm, m2_hbm,
    nw, n1, n2, gfin, gc_out,
    wv, ctx, ctxt_all, ctxt, cot, gain_flat, gain, psend, precv, own, stat_s, stat_r, inverse_v, shift_v, g4, gx,
    sends, recvs, keeps, fsend, frecv, fkeep, m1, m2, master, gc_acc,
    gp, gpr,
    in_sem, w_sem, cot_sem, m_sem,
    ps_s, ps_r, st_s, st_r, cx_s, cx_r, gy_s, gx_s, gx_r, gm_s, gm_r,
    rs_s, rs_r, fx_s, fx_r, gg_s, gg_r,
):
    n, bits, quarter, cw, rows, tok, heads, width = cfg
    half = 2 * quarter
    chunks = 4 * quarter
    stages = bits - 2
    dp, mp = lax.axis_index("dp"), lax.axis_index("mp")
    peer = 1 - mp
    side = (dp // 2) % 2
    order = [*range(2, bits), 1]

    def flip(index, bit):
        return index + (1 << bit) * (1 - 2 * ((index // (1 << bit)) % 2))

    def peer_id():
        return (dp, peer)

    def bit_id(bit):
        return (flip(dp, bit), mp)

    starts = [
        (2 * y_half + x_side) * quarter
        for x_side in (side, 1 - side) for y_half in (mp, peer)
    ]

    def cols(group, j):
        return pl.ds(pl.multiple_of((starts[group] + j) * cw, cw), cw)

    def cols_of(across, i):
        near, far = starts[2 * across:2 * across + 2]
        first = jnp.where(i < quarter, near + i, far + i - quarter)
        return pl.ds(pl.multiple_of(first * cw, cw), cw)

    def ctx_copy():
        return pltpu.make_async_copy(ctx_hbm, ctx.at[pl.ds(0, tok)], in_sem.at[0])

    def gain_copy():
        return pltpu.make_async_copy(gain_hbm, gain_flat, in_sem.at[1])

    def w_copy(group, j, sem):
        base = half * (1 - group % 2)
        return pltpu.make_async_copy(
            w_hbm.at[:, cols(group, j)], wv.at[base + 2 * j + group // 2], sem
        )

    def w_wait(first, last, sem):
        block = wv.at[pl.ds(first, last - first)]
        pltpu.make_async_copy(block, block, sem).wait()

    def cot_copy(far, j):
        h = far * quarter + j
        return pltpu.make_async_copy(cot_hbm.at[:, cols(2 * far, j)], cot.at[h], cot_sem)

    def m_copies():
        return (
            pltpu.make_async_copy(m1_hbm.at[0], m1, m_sem.at[0]),
            pltpu.make_async_copy(m2_hbm.at[0], m2, m_sem.at[1]),
            pltpu.make_async_copy(
                w_hbm.at[pl.ds(pl.multiple_of(dp * rows, rows), rows), :], master, m_sem.at[2]
            ),
        )

    def remote(src, dst, send_sem, recv_sem, device):
        return pltpu.make_async_remote_copy(
            src_ref=src, dst_ref=dst, send_sem=send_sem, recv_sem=recv_sem,
            device_id=device, device_id_type=MESH,
        )

    def partial_send(h):
        return remote(psend.at[h], precv.at[h], ps_s, ps_r.at[h], peer_id())

    def stat_send():
        return remote(stat_s, stat_r, st_s, st_r, peer_id())

    def ctx_send(a, b, i, bit):
        return remote(
            ctx.at[pl.ds(a * tok, tok)], ctx.at[pl.ds(b * tok, tok)], cx_s, cx_r.at[i], bit_id(bit)
        )

    def ctx_mate():
        return ctx_send(0, 1, 0, 0)

    def ctx_side():
        return ctx_send(0, 2, 1, 1)

    def ctx_relay():
        return ctx_send(2, 3, 2, 0)

    def grad_peer_near(j):
        return remote(
            g4.at[j, pl.ds(0, tok)], g4.at[quarter + j, pl.ds(0, tok)],
            gy_s.at[0], ps_r.at[j], peer_id(),
        )

    def grad_peer_far(j):
        return remote(
            gx.at[j], gx.at[quarter + j], gy_s.at[1], ps_r.at[quarter + j], peer_id()
        )

    def grad_side(i):
        return remote(gx.at[i], g4.at[i, pl.ds(2 * tok, tok)], gx_s, gx_r.at[i], bit_id(1))

    def grad_mate(i):
        return remote(
            g4.at[i, pl.ds(0, tok)], g4.at[i, pl.ds(tok, tok)], gm_s.at[0], gm_r.at[i], bit_id(0)
        )

    def grad_relay(i):
        return remote(
            g4.at[i, pl.ds(2 * tok, tok)], g4.at[i, pl.ds(3 * tok, tok)],
            gm_s.at[1], gm_r.at[i], bit_id(0),
        )

    def grad_chip(i):
        both = g4.at[i, pl.ds(0, 2 * tok)]
        return remote(both, both, gm_s.at[0], gm_r.at[i], bit_id(0))

    def shard_send(s, i):
        return remote(
            sends[s].at[i], recvs[s].at[i], rs_s.at[s], rs_r.at[s, i], bit_id(order[s])
        )

    def swap_send(i):
        other = jnp.where(i < 2, 1 - i, i)
        return remote(fsend.at[i], frecv.at[other], fx_s, fx_r.at[other], bit_id(1))

    def swap_wait(i):
        remote(fsend.at[i], frecv.at[i], fx_s, fx_r.at[i], bit_id(1)).wait_recv()

    steps = [0, *order]

    def gain_send(b):
        device = bit_id(steps[b]) if b < bits else peer_id()
        return remote(gp.at[b], gpr.at[b], gg_s, gg_r.at[b], device)

    barrier = pltpu.get_barrier_semaphore()
    pl.semaphore_signal(barrier, inc=1, device_id=peer_id(), device_id_type=MESH)
    for bit in range(bits - 1, -1, -1):
        pl.semaphore_signal(barrier, inc=1, device_id=bit_id(bit), device_id_type=MESH)

    ctx_copy().start()
    w_copy(1, 0, w_sem.at[0]).start()
    w_copy(3, 0, w_sem.at[0]).start()

    def pair(base, j):
        right = jnp.concatenate([wv[base + 2 * j], wv[base + 2 * j + 1]], axis=1)
        return jnp.dot(ctx[0:tok], right, preferred_element_type=F32)

    def partial(j):
        value = pair(0, j).astype(BF16)
        psend[j] = value[:, :cw]
        psend[quarter + j] = value[:, cw:]

    def partial_start(j):
        partial_send(j).start()
        partial_send(quarter + j).start()

    ctx_copy().wait()
    w_wait(0, 2, w_sem.at[0])

    @pl.loop(1, quarter)
    def _(j):
        w_copy(1, j, w_sem.at[1]).start()
        w_copy(3, j, w_sem.at[1]).start()

    @pl.loop(0, quarter)
    def _(j):
        w_copy(0, j, w_sem.at[2]).start()
        w_copy(2, j, w_sem.at[2]).start()

    partial(0)
    pl.semaphore_wait(barrier, bits + 1)

    partial_start(0)
    w_wait(2, half, w_sem.at[1])

    @pl.loop(1, quarter)
    def _(j):
        partial(j)
        partial_start(j)
        cot_copy(0, j).start()
        cot_copy(1, j).start()

    ctx_side().start()
    ctx_mate().start()
    cot_copy(0, 0).start()
    cot_copy(1, 0).start()
    gain_copy().start()
    w_wait(half, chunks, w_sem.at[2])

    @pl.loop(0, quarter)
    def _(j):
        value = pair(half, j)
        own[j] = value[:, :cw]
        own[quarter + j] = value[:, cw:]

    for copy in m_copies():
        copy.start()

    gain_copy().wait()
    for r in range(chunks):
        gain[r] = gain_flat[r * cw:(r + 1) * cw].reshape(1, cw)

    def turn(p):
        ctxt_all[...] = jnp.transpose(
            ctx[2 * p * tok:2 * (p + 1) * tok].astype(F32)
        ).reshape(n, rows, 2 * tok)
        blocks = []
        for spot in range(n // 2):
            shard = dp
            for i, k in enumerate(order):
                if not (spot >> (bits - 2 - i)) & 1:
                    shard = flip(shard, k)
            blocks.append(ctxt_all[shard])
        ctxt[p] = jnp.concatenate(blocks, axis=0).astype(BF16)

    pltpu.make_async_copy(cot, cot, cot_sem).wait()
    ctx_mate().wait_recv()
    turn(0)

    def gather_stats(far, j, carry):
        square, cross = carry
        h = far * quarter + j
        partial_send(h).wait_recv()
        attn = own[h] + precv[h].astype(F32)
        own[h] = attn
        scaled = cot[h].astype(F32) * gain[starts[2 * far] + j]
        return square + attn * attn, cross + scaled * attn

    def gather_pair(j, carry):
        return gather_stats(1, j, gather_stats(0, j, carry))

    early, late = (2 * quarter) // 3, (5 * quarter) // 6
    zero = jnp.zeros((tok, cw), F32)
    carry = lax.fori_loop(0, early, gather_pair, (zero, zero))
    ctx_side().wait_recv()
    ctx_relay().start()
    carry = lax.fori_loop(early, late, gather_pair, carry)
    ctx_relay().wait_recv()
    turn(1)
    square, cross = lax.fori_loop(late, quarter, gather_pair, carry)
    square = jnp.sum(square, axis=1, keepdims=True)
    cross = jnp.sum(cross, axis=1, keepdims=True)
    even = lax.broadcasted_iota(jnp.int32, (tok, 128), 1) % 2 == 0
    stat_s[...] = jnp.transpose(jnp.where(even, square, cross))[0:8]
    stat_send().start()
    stat_send().wait_recv()
    totals = stat_s[...] + stat_r[...]

    def spread(row):
        return jnp.transpose(jnp.concatenate([totals[row:row + 1]] * 128, axis=0))

    inverse = lax.rsqrt(spread(0) / width + norm_floor)
    inverse_v[...] = inverse
    shift_v[...] = inverse * spread(1) / width

    def gradient(far, j):
        h = far * quarter + j
        spot = starts[2 * far] + j
        inverse = inverse_v[...]
        upstream = cot[h].astype(F32)
        normed = own[h] * inverse
        gp[0, spot - half * mp] = jnp.sum(upstream * normed, axis=0, keepdims=True)
        return (inverse * (upstream * gain[spot] - normed * shift_v[...])).astype(BF16)

    gx[0] = gradient(1, 0)
    g4[0, 2 * tok:3 * tok] = gx[0]
    grad_relay(0).start()
    grad_peer_far(0).start()
    g4[0, 0:tok] = gradient(0, 0)
    grad_mate(0).start()

    def far_part(j):
        gx[j] = gradient(1, j)
        grad_side(j).start()
        grad_peer_far(j).start()

    @pl.loop(1, FIRST)
    def _(j):
        far_part(j)

    @pl.loop(1, quarter)
    def _(j):
        g4[j, 0:tok] = gradient(0, j)
        grad_mate(j).start()

    def context_part(u, base):
        left = jnp.concatenate([g4[u, 0:tok], gx[u]], axis=1)
        right = jnp.concatenate([wv[base], wv[base + 1]], axis=1)
        return lax.dot_general(left, right, (((1,), (1,)), ((), ())), preferred_element_type=F32)

    gc_acc[...] = context_part(0, half)

    @pl.loop(FIRST, quarter)
    def _(j):
        far_part(j)

    gain_send(0).start()

    @pl.loop(0, quarter)
    def _(j):
        grad_peer_near(j).start()

    def context_add(u):
        gc_acc[...] += context_part(u, half + 2 * u)

    @pl.loop(1, WARM)
    def _(u):
        context_add(u)

    def split(slot, product):
        cut = product.shape[0] // 2
        sends[0][slot] = product[:cut].astype(BF16)
        shard_send(0, slot).start()
        keeps[0][slot] = product[cut:]

    grad_chip(0).wait_recv()
    for slot in range(2):
        split(slot, jnp.dot(
            ctxt[0], g4[0, 2 * slot * tok:2 * (slot + 1) * tok], preferred_element_type=F32
        ))

    @pl.loop(WARM, quarter)
    def _(u):
        context_add(u)

    def adam(total, cols):
        first = beta_one * m1[:, cols] + (1.0 - beta_one) * total
        second = beta_two * m2[:, cols] + (1.0 - beta_two) * total * total
        nw[0, :, cols] = (
            master[:, cols].astype(F32) - learn_rate * first / (jnp.sqrt(second) + adam_floor)
        ).astype(BF16)
        n1[0, :, cols] = first
        n2[0, :, cols] = second

    for copy in m_copies():
        copy.wait()

    swap_lag = LAG * stages + SWAP

    @pl.loop(1, max(half + swap_lag, 3 * bits + 6))
    def _(t):
        @pl.when(t < half)
        def _():
            grad_side(t).wait_recv()
            grad_relay(t).start()

        @pl.when((t >= quarter) & (t < half))
        def _():
            grad_peer_near(t - quarter).wait_recv()
            grad_mate(t).start()
            gc_acc[...] += context_part(t, 2 * (t - quarter))

        @pl.when(t == half)
        def _():
            gc_out[...] = gc_acc[...].astype(BF16)

        for b in range(bits + 1):
            @pl.when(t == 3 * b + 1 + 3 * (b >= bits - 1) + (b == bits))
            def _():
                gain_send(b).wait_recv()
                if b < bits:
                    gp[b + 1] = gp[b] + gpr[b]
                    gain_send(b + 1).start()
                else:
                    gfin[pl.ds(mp * half, half)] = gp[bits]
                    gfin[pl.ds(peer * half, half)] = gpr[bits]

        late_swap = t + 1 - swap_lag

        @pl.when((late_swap >= 0) & (late_swap <= half))
        def _():
            swap_wait(late_swap)
            total = frecv[late_swap].astype(F32)

            @pl.when(late_swap < 2)
            def _():
                first = jnp.where(late_swap == 0, starts[0], starts[2])
                adam(total + fkeep[late_swap], pl.ds(pl.multiple_of(first * cw, cw), cw))

            @pl.when(late_swap >= 2)
            def _():
                adam(total, cols_of(1, late_swap - 1))

        for s in range(stages - 1, -1, -1):
            i = t + 1 - LAG * (s + 1)

            @pl.when((i >= 0) & (i <= half))
            def _():
                shard_send(s, i).wait_recv()
                total = keeps[s][i] + recvs[s][i].astype(F32)
                cut = total.shape[0] // 2
                if s < stages - 1:
                    sends[s + 1][i] = total[:cut].astype(BF16)
                    shard_send(s + 1, i).start()
                    keeps[s + 1][i] = total[cut:]
                else:
                    fsend[i] = total[:cut].astype(BF16)
                    swap_send(i).start()

                    @pl.when(i < 2)
                    def _():
                        fkeep[i] = total[cut:]

                    @pl.when(i >= 2)
                    def _():
                        adam(total[cut:], cols_of(0, i - 1))

        @pl.when(t < half)
        def _():
            grad_chip(t).wait_recv()
            product = jnp.dot(ctxt[0], g4[t, 0:2 * tok], preferred_element_type=F32)
            product += jnp.dot(ctxt[1], g4[t, 2 * tok:4 * tok], preferred_element_type=F32)
            split(t + 1, product)

        @pl.when(t <= quarter)
        def _():
            grad_peer_far(t - 1).wait_recv()
            grad_side(quarter + t - 1).start()

    def drain(block, sem):
        remote(block, block, sem, st_r, peer_id()).wait_send()

    stat_send().wait_send()
    drain(ctx.at[pl.ds(0, 3 * tok)], cx_s)
    drain(psend, ps_s)
    drain(gx.at[pl.ds(0, quarter)], gy_s.at[0])
    drain(gx.at[pl.ds(0, quarter)], gy_s.at[1])
    drain(gx.at[pl.ds(0, half - 1)], gx_s)
    drain(gx, gm_s.at[0])
    drain(gx, gm_s.at[1])
    drain(gp, gg_s)
    drain(fsend, fx_s)
    for s in range(stages):
        drain(sends[s], rs_s.at[s])


def settle(nw, n1, n2, gg, gc, nw_out, n1_out, n2_out, gg_out, gc_out, flat, sem):
    pairs = ((nw, nw_out), (n1, n1_out), (n2, n2_out), (gc, gc_out))
    copies = [pltpu.make_async_copy(a, b, sem.at[i]) for i, (a, b) in enumerate(pairs)]
    for copy in copies:
        copy.start()
    chunks, _, cw = gg.shape
    for r in range(chunks):
        flat[r * cw:(r + 1) * cw] = gg[r].reshape(cw)
    copies.append(pltpu.make_async_copy(flat, gg_out, sem.at[4]))
    copies[-1].start()
    for copy in copies:
        copy.wait()


def per_device(n, context, out_weight, cotangent, norm_gain, first_moment, second_moment):
    tok, heads = context.shape
    width = out_weight.shape[1]
    rows = first_moment.shape[1]
    bits = n.bit_length() - 1
    cw = 128
    quarter = width // (4 * cw)
    half, chunks = 2 * quarter, 4 * quarter
    stages = bits - 2
    cfg = (n, bits, quarter, cw, rows, tok, heads, width)
    sizes = [(n >> (s + 2)) * rows for s in range(stages)]
    dma = pltpu.SemaphoreType.DMA
    vmem = pltpu.VMEM
    scratch = [
        vmem((chunks, heads, cw), BF16),
        vmem((4 * tok, heads), BF16),
        vmem((n, rows, 2 * tok), F32),
        vmem((2, heads // 2, 2 * tok), BF16),
        vmem((half, tok, cw), BF16),
        vmem((width,), F32),
        vmem((chunks, 1, cw), F32),
        vmem((half, tok, cw), BF16),
        vmem((half, tok, cw), BF16),
        vmem((half, tok, cw), F32),
        vmem((8, tok), F32),
        vmem((8, tok), F32),
        vmem((tok, cw), F32),
        vmem((tok, cw), F32),
        vmem((half, 4 * tok, cw), BF16),
        vmem((half, tok, cw), BF16),
        tuple(vmem((half + 1, size, cw), BF16) for size in sizes),
        tuple(vmem((half + 1, size, cw), BF16) for size in sizes),
        tuple(vmem((half + 1, size, cw), F32) for size in sizes),
        vmem((half + 1, rows, cw), BF16),
        vmem((half + 1, rows, cw), BF16),
        vmem((2, rows, cw), F32),
        vmem((rows, width), F32),
        vmem((rows, width), F32),
        vmem((rows, width), BF16),
        vmem((tok, heads), F32),
        vmem((bits + 1, half, 1, cw), F32),
        vmem((bits + 1, half, 1, cw), F32),
        dma((2,)), dma((3,)), dma, dma((3,)),
        dma, dma((half,)), dma, dma, dma, dma((3,)),
        dma((2,)), dma, dma((half,)), dma((2,)), dma((half,)),
        dma((stages,)), dma((stages, half + 1)), dma, dma((half + 1,)),
        dma, dma((bits + 1,)),
    ]
    anywhere = pl.BlockSpec(memory_space=pltpu.HBM)
    pin = functools.partial(pltpu.with_memory_space_constraint, memory_space=pltpu.HBM)
    new_weight, new_first, new_second, grad_gain, grad_context = pl.pallas_call(
        functools.partial(kernel, cfg),
        out_shape=(
            jax.ShapeDtypeStruct(first_moment.shape, BF16),
            jax.ShapeDtypeStruct(first_moment.shape, F32),
            jax.ShapeDtypeStruct(first_moment.shape, F32),
            jax.ShapeDtypeStruct((chunks, 1, cw), F32),
            jax.ShapeDtypeStruct((tok, heads), BF16),
        ),
        in_specs=[anywhere] * 6,
        out_specs=(pl.BlockSpec(memory_space=pltpu.VMEM),) * 5,
        scratch_shapes=scratch,
        compiler_params=pltpu.CompilerParams(
            collective_id=0, has_side_effects=True, vmem_limit_bytes=VMEM_LIMIT
        ),
    )(*map(pin, (context, out_weight, cotangent, norm_gain, first_moment, second_moment)))
    return pl.pallas_call(
        settle,
        out_shape=(
            jax.ShapeDtypeStruct(first_moment.shape, BF16),
            jax.ShapeDtypeStruct(first_moment.shape, F32),
            jax.ShapeDtypeStruct(first_moment.shape, F32),
            jax.ShapeDtypeStruct((width,), F32),
            jax.ShapeDtypeStruct((tok, heads), BF16),
        ),
        in_specs=[pl.BlockSpec(memory_space=pltpu.VMEM)] * 5,
        out_specs=(anywhere,) * 5,
        scratch_shapes=[vmem((width,), F32), dma((5,))],
        compiler_params=pltpu.CompilerParams(vmem_limit_bytes=8 * 1024 * 1024),
    )(new_weight, new_first, new_second, grad_gain, grad_context)


def solution(mesh):
    return jax.shard_map(
        functools.partial(per_device, mesh.shape["dp"]),
        mesh=mesh,
        in_specs=(
            P("dp", "mp"),
            P("mp", None),
            P("dp", None),
            P(),
            P("mp", "dp", None),
            P("mp", "dp", None),
        ),
        out_specs=(
            P("mp", "dp", None),
            P("mp", "dp", None),
            P("mp", "dp", None),
            P(),
            P("dp", "mp"),
        ),
        check_vma=False,
    )
```

```python
import functools

import jax
import jax.numpy as jnp
from jax import lax
from jax.experimental import pallas as pl
from jax.experimental.pallas import tpu as pltpu
from jax.sharding import PartitionSpec as P

norm_floor = 0.1
learn_rate = 0.01
beta_one = 0.9
beta_two = 0.95
adam_floor = 1e-08

MESH = pl.DeviceIdType.MESH
F32 = jnp.float32
BF16 = jnp.bfloat16
VMEM_LIMIT = 50 * 1024 * 1024
LAG = 3
SWAP = 6
FIRST = 2
WARM = 3
MERGE = 4


def kernel(
    cfg,
    ctx_hbm, w_hbm, cot_hbm, gain_hbm, m1_hbm, m2_hbm,
    nw, n1, n2, gfin, gc_out,
    wv, ctx, ctxt_all, ctxt, cot, gain_flat, gain, psend, precv, own, stat_s, stat_r, inverse_v, shift_v, g4, gx,
    sends, recvs, keeps, fsend, frecv, fkeep, m1, m2, master, gc_acc,
    gp, gpr,
    in_sem, w_sem, cot_sem, m_sem,
    ps_s, ps_r, st_s, st_r, cx_s, cx_r, gy_s, gx_s, gx_r, gm_s, gm_r,
    rs_s, rs_r, fx_s, fx_r, gg_s, gg_r,
):
    n, bits, quarter, cw, rows, tok, heads, width = cfg
    half = 2 * quarter
    chunks = 4 * quarter
    stages = bits - 2
    merged = half + 1 - MERGE
    dp, mp = lax.axis_index("dp"), lax.axis_index("mp")
    peer = 1 - mp
    side = (dp // 2) % 2
    order = [*range(2, bits), 1]

    def flip(index, bit):
        return index + (1 << bit) * (1 - 2 * ((index // (1 << bit)) % 2))

    def peer_id():
        return (dp, peer)

    def bit_id(bit):
        return (flip(dp, bit), mp)

    starts = [
        (2 * y_half + x_side) * quarter
        for x_side in (side, 1 - side) for y_half in (mp, peer)
    ]

    def cols(group, j):
        return pl.ds(pl.multiple_of((starts[group] + j) * cw, cw), cw)

    def cols_of(across, i):
        near, far = starts[2 * across:2 * across + 2]
        first = jnp.where(i < quarter, near + i, far + i - quarter)
        return pl.ds(pl.multiple_of(first * cw, cw), cw)

    def ctx_copy():
        return pltpu.make_async_copy(ctx_hbm, ctx.at[pl.ds(0, tok)], in_sem.at[0])

    def gain_copy():
        return pltpu.make_async_copy(gain_hbm, gain_flat, in_sem.at[1])

    def w_copy(group, j, sem):
        base = half * (1 - group % 2)
        return pltpu.make_async_copy(
            w_hbm.at[:, cols(group, j)], wv.at[base + 2 * j + group // 2], sem
        )

    def w_wait(first, last, sem):
        block = wv.at[pl.ds(first, last - first)]
        pltpu.make_async_copy(block, block, sem).wait()

    def cot_copy(far, j):
        h = far * quarter + j
        return pltpu.make_async_copy(cot_hbm.at[:, cols(2 * far, j)], cot.at[h], cot_sem)

    def m_copies():
        return (
            pltpu.make_async_copy(m1_hbm.at[0], m1, m_sem.at[0]),
            pltpu.make_async_copy(m2_hbm.at[0], m2, m_sem.at[1]),
            pltpu.make_async_copy(
                w_hbm.at[pl.ds(pl.multiple_of(dp * rows, rows), rows), :], master, m_sem.at[2]
            ),
        )

    def remote(src, dst, send_sem, recv_sem, device):
        return pltpu.make_async_remote_copy(
            src_ref=src, dst_ref=dst, send_sem=send_sem, recv_sem=recv_sem,
            device_id=device, device_id_type=MESH,
        )

    def partial_send(h):
        return remote(psend.at[h], precv.at[h], ps_s, ps_r.at[h], peer_id())

    def stat_send():
        return remote(stat_s, stat_r, st_s, st_r, peer_id())

    def ctx_send(a, b, i, bit):
        return remote(
            ctx.at[pl.ds(a * tok, tok)], ctx.at[pl.ds(b * tok, tok)], cx_s, cx_r.at[i], bit_id(bit)
        )

    def ctx_mate():
        return ctx_send(0, 1, 0, 0)

    def ctx_side():
        return ctx_send(0, 2, 1, 1)

    def ctx_relay():
        return ctx_send(2, 3, 2, 0)

    def grad_peer_near(j):
        return remote(
            g4.at[j, pl.ds(0, tok)], g4.at[quarter + j, pl.ds(0, tok)],
            gy_s.at[0], ps_r.at[j], peer_id(),
        )

    def grad_peer_far(j):
        return remote(
            gx.at[j], gx.at[quarter + j], gy_s.at[1], ps_r.at[quarter + j], peer_id()
        )

    def grad_side(i):
        return remote(gx.at[i], g4.at[i, pl.ds(2 * tok, tok)], gx_s, gx_r.at[i], bit_id(1))

    def grad_mate(i):
        return remote(
            g4.at[i, pl.ds(0, tok)], g4.at[i, pl.ds(tok, tok)], gm_s.at[0], gm_r.at[i], bit_id(0)
        )

    def grad_relay(i):
        return remote(
            g4.at[i, pl.ds(2 * tok, tok)], g4.at[i, pl.ds(3 * tok, tok)],
            gm_s.at[1], gm_r.at[i], bit_id(0),
        )

    def grad_chip(i):
        both = g4.at[i, pl.ds(0, 2 * tok)]
        return remote(both, both, gm_s.at[0], gm_r.at[i], bit_id(0))

    def shard_send(s, i):
        return remote(
            sends[s].at[i], recvs[s].at[i], rs_s.at[s], rs_r.at[s, i], bit_id(order[s])
        )

    def last_send(i, across):
        part = pl.ds(rows * (1 - across), rows)
        device = flip(dp, order[stages - 1])
        return remote(
            sends[-1].at[i, part], recvs[-1].at[i, part], rs_s.at[stages - 1], rs_r.at[stages - 1, i],
            (flip(device, 1) if across else device, mp),
        )

    def swap_send(i):
        other = jnp.where(i < 2, 1 - i, i)
        return remote(fsend.at[i], frecv.at[other], fx_s, fx_r.at[other], bit_id(1))

    def swap_wait(i):
        remote(fsend.at[i], frecv.at[i], fx_s, fx_r.at[i], bit_id(1)).wait_recv()

    steps = [0, *order]

    def gain_send(b):
        device = bit_id(steps[b]) if b < bits else peer_id()
        return remote(gp.at[b], gpr.at[b], gg_s, gg_r.at[b], device)

    barrier = pltpu.get_barrier_semaphore()
    pl.semaphore_signal(barrier, inc=1, device_id=peer_id(), device_id_type=MESH)
    for bit in range(bits - 1, -1, -1):
        pl.semaphore_signal(barrier, inc=1, device_id=bit_id(bit), device_id_type=MESH)

    diagonal = (flip(flip(dp, order[stages - 1]), 1), mp)
    pl.semaphore_signal(barrier, inc=1, device_id=diagonal, device_id_type=MESH)

    ctx_copy().start()
    w_copy(1, 0, w_sem.at[0]).start()
    w_copy(3, 0, w_sem.at[0]).start()

    def pair(base, j):
        right = jnp.concatenate([wv[base + 2 * j], wv[base + 2 * j + 1]], axis=1)
        return jnp.dot(ctx[0:tok], right, preferred_element_type=F32)

    def partial(j):
        value = pair(0, j).astype(BF16)
        psend[j] = value[:, :cw]
        psend[quarter + j] = value[:, cw:]

    def partial_start(j):
        partial_send(j).start()
        partial_send(quarter + j).start()

    ctx_copy().wait()
    w_wait(0, 2, w_sem.at[0])

    @pl.loop(1, quarter)
    def _(j):
        w_copy(1, j, w_sem.at[1]).start()
        w_copy(3, j, w_sem.at[1]).start()

    @pl.loop(0, quarter)
    def _(j):
        w_copy(0, j, w_sem.at[2]).start()
        w_copy(2, j, w_sem.at[2]).start()

    partial(0)
    pl.semaphore_wait(barrier, bits + 2)

    partial_start(0)
    w_wait(2, half, w_sem.at[1])

    @pl.loop(1, quarter)
    def _(j):
        partial(j)
        partial_start(j)
        cot_copy(0, j).start()
        cot_copy(1, j).start()

    ctx_side().start()
    ctx_mate().start()
    cot_copy(0, 0).start()
    cot_copy(1, 0).start()
    gain_copy().start()
    w_wait(half, chunks, w_sem.at[2])

    @pl.loop(0, quarter)
    def _(j):
        value = pair(half, j)
        own[j] = value[:, :cw]
        own[quarter + j] = value[:, cw:]

    for copy in m_copies():
        copy.start()

    gain_copy().wait()
    for r in range(chunks):
        gain[r] = gain_flat[r * cw:(r + 1) * cw].reshape(1, cw)

    def turn(p):
        ctxt_all[...] = jnp.transpose(
            ctx[2 * p * tok:2 * (p + 1) * tok].astype(F32)
        ).reshape(n, rows, 2 * tok)
        blocks = []
        for spot in range(n // 2):
            shard = dp
            for i, k in enumerate(order):
                if not (spot >> (bits - 2 - i)) & 1:
                    shard = flip(shard, k)
            blocks.append(ctxt_all[shard])
        ctxt[p] = jnp.concatenate(blocks, axis=0).astype(BF16)

    pltpu.make_async_copy(cot, cot, cot_sem).wait()
    ctx_mate().wait_recv()
    turn(0)

    def gather_stats(far, j, carry):
        square, cross = carry
        h = far * quarter + j
        partial_send(h).wait_recv()
        attn = own[h] + precv[h].astype(F32)
        own[h] = attn
        scaled = cot[h].astype(F32) * gain[starts[2 * far] + j]
        return square + attn * attn, cross + scaled * attn

    def gather_pair(j, carry):
        return gather_stats(1, j, gather_stats(0, j, carry))

    early, late = (2 * quarter) // 3, (5 * quarter) // 6
    zero = jnp.zeros((tok, cw), F32)
    carry = lax.fori_loop(0, early, gather_pair, (zero, zero))
    ctx_side().wait_recv()
    ctx_relay().start()
    carry = lax.fori_loop(early, late, gather_pair, carry)
    ctx_relay().wait_recv()
    turn(1)
    square, cross = lax.fori_loop(late, quarter, gather_pair, carry)
    square = jnp.sum(square, axis=1, keepdims=True)
    cross = jnp.sum(cross, axis=1, keepdims=True)
    even = lax.broadcasted_iota(jnp.int32, (tok, 128), 1) % 2 == 0
    stat_s[...] = jnp.transpose(jnp.where(even, square, cross))[0:8]
    stat_send().start()
    stat_send().wait_recv()
    totals = stat_s[...] + stat_r[...]

    def spread(row):
        return jnp.transpose(jnp.concatenate([totals[row:row + 1]] * 128, axis=0))

    inverse = lax.rsqrt(spread(0) / width + norm_floor)
    inverse_v[...] = inverse
    shift_v[...] = inverse * spread(1) / width

    def gradient(far, j):
        h = far * quarter + j
        spot = starts[2 * far] + j
        inverse = inverse_v[...]
        upstream = cot[h].astype(F32)
        normed = own[h] * inverse
        gp[0, spot - half * mp] = jnp.sum(upstream * normed, axis=0, keepdims=True)
        return (inverse * (upstream * gain[spot] - normed * shift_v[...])).astype(BF16)

    gx[0] = gradient(1, 0)
    g4[0, 2 * tok:3 * tok] = gx[0]
    grad_relay(0).start()
    grad_peer_far(0).start()
    g4[0, 0:tok] = gradient(0, 0)
    grad_mate(0).start()

    def far_part(j):
        gx[j] = gradient(1, j)
        grad_side(j).start()
        grad_peer_far(j).start()

    @pl.loop(1, FIRST)
    def _(j):
        far_part(j)

    @pl.loop(1, quarter)
    def _(j):
        g4[j, 0:tok] = gradient(0, j)
        grad_mate(j).start()

    def context_part(u, base):
        left = jnp.concatenate([g4[u, 0:tok], gx[u]], axis=1)
        right = jnp.concatenate([wv[base], wv[base + 1]], axis=1)
        return lax.dot_general(left, right, (((1,), (1,)), ((), ())), preferred_element_type=F32)

    gc_acc[...] = context_part(0, half)

    @pl.loop(FIRST, quarter)
    def _(j):
        far_part(j)

    gain_send(0).start()

    @pl.loop(0, quarter)
    def _(j):
        grad_peer_near(j).start()

    def context_add(u):
        gc_acc[...] += context_part(u, half + 2 * u)

    warm = 1 + (WARM - 1) * (dp % 2)

    @pl.loop(1, warm)
    def _(u):
        context_add(u)

    def split(slot, product):
        cut = product.shape[0] // 2
        sends[0][slot] = product[:cut].astype(BF16)
        shard_send(0, slot).start()
        keeps[0][slot] = product[cut:]

    grad_chip(0).wait_recv()
    for slot in range(2):
        split(slot, jnp.dot(
            ctxt[0], g4[0, 2 * slot * tok:2 * (slot + 1) * tok], preferred_element_type=F32
        ))

    @pl.loop(warm, quarter)
    def _(u):
        context_add(u)

    def adam(total, cols):
        first = beta_one * m1[:, cols] + (1.0 - beta_one) * total
        second = beta_two * m2[:, cols] + (1.0 - beta_two) * total * total
        nw[0, :, cols] = (
            master[:, cols].astype(F32) - learn_rate * first / (jnp.sqrt(second) + adam_floor)
        ).astype(BF16)
        n1[0, :, cols] = first
        n2[0, :, cols] = second

    for copy in m_copies():
        copy.wait()

    swap_lag = LAG * stages + SWAP

    @pl.loop(1, max(half + swap_lag, 3 * bits + 6))
    def _(t):
        @pl.when(t < half)
        def _():
            grad_side(t).wait_recv()
            grad_relay(t).start()

        @pl.when((t >= quarter) & (t < half))
        def _():
            grad_peer_near(t - quarter).wait_recv()
            grad_mate(t).start()
            gc_acc[...] += context_part(t, 2 * (t - quarter))

        @pl.when(t == half)
        def _():
            gc_out[...] = gc_acc[...].astype(BF16)

        for b in range(bits + 1):
            @pl.when(t == 3 * b + 1 + 3 * (b >= bits - 1) + (b == bits))
            def _():
                gain_send(b).wait_recv()
                if b < bits:
                    gp[b + 1] = gp[b] + gpr[b]
                    gain_send(b + 1).start()
                else:
                    gfin[pl.ds(mp * half, half)] = gp[bits]
                    gfin[pl.ds(peer * half, half)] = gpr[bits]

        late_swap = t + 1 - swap_lag

        @pl.when((late_swap >= 0) & (late_swap <= half))
        def _():
            swap_wait(late_swap)
            total = frecv[late_swap].astype(F32)

            @pl.when(late_swap < 2)
            def _():
                first = jnp.where(late_swap == 0, starts[0], starts[2])
                adam(total + fkeep[late_swap], pl.ds(pl.multiple_of(first * cw, cw), cw))

            @pl.when((late_swap >= 2) & (late_swap < merged))
            def _():
                adam(total, cols_of(1, late_swap - 1))

            @pl.when(late_swap >= merged)
            def _():
                adam(total + recvs[-1][late_swap, 0:rows].astype(F32), cols_of(1, late_swap - 1))

        for s in range(stages - 1, -1, -1):
            i = t + 1 - LAG * (s + 1)

            @pl.when((i >= 0) & (i <= half))
            def _():
                shard_send(s, i).wait_recv()
                total = keeps[s][i] + recvs[s][i].astype(F32)
                cut = total.shape[0] // 2
                if s < stages - 1:
                    sends[s + 1][i] = total[:cut].astype(BF16)
                    if s < stages - 2:
                        shard_send(s + 1, i).start()
                    else:
                        @pl.when(i < merged)
                        def _():
                            shard_send(s + 1, i).start()

                        @pl.when(i >= merged)
                        def _():
                            last_send(i, 1).start()
                            last_send(i, 0).start()
                            fsend[i] = total[cut:cut + rows].astype(BF16)
                            swap_send(i).start()

                    keeps[s + 1][i] = total[cut:]
                else:
                    @pl.when(i < merged)
                    def _():
                        fsend[i] = total[:cut].astype(BF16)
                        swap_send(i).start()

                    @pl.when(i < 2)
                    def _():
                        fkeep[i] = total[cut:]

                    @pl.when(i >= 2)
                    def _():
                        adam(total[cut:], cols_of(0, i - 1))

        @pl.when(t < half)
        def _():
            grad_chip(t).wait_recv()
            product = jnp.dot(ctxt[0], g4[t, 0:2 * tok], preferred_element_type=F32)
            product += jnp.dot(ctxt[1], g4[t, 2 * tok:4 * tok], preferred_element_type=F32)
            split(t + 1, product)

        @pl.when(t <= quarter)
        def _():
            grad_peer_far(t - 1).wait_recv()
            grad_side(quarter + t - 1).start()

    def drain(block, sem):
        remote(block, block, sem, st_r, peer_id()).wait_send()

    stat_send().wait_send()
    drain(ctx.at[pl.ds(0, 3 * tok)], cx_s)
    drain(psend, ps_s)
    drain(gx.at[pl.ds(0, quarter)], gy_s.at[0])
    drain(gx.at[pl.ds(0, quarter)], gy_s.at[1])
    drain(gx.at[pl.ds(0, half - 1)], gx_s)
    drain(gx, gm_s.at[0])
    drain(gx, gm_s.at[1])
    drain(gp, gg_s)
    drain(fsend, fx_s)
    for s in range(stages):
        drain(sends[s], rs_s.at[s])


def settle(nw, n1, n2, gg, gc, nw_out, n1_out, n2_out, gg_out, gc_out, flat, sem):
    pairs = ((nw, nw_out), (n1, n1_out), (n2, n2_out), (gc, gc_out))
    copies = [pltpu.make_async_copy(a, b, sem.at[i]) for i, (a, b) in enumerate(pairs)]
    for copy in copies:
        copy.start()
    chunks, _, cw = gg.shape
    for r in range(chunks):
        flat[r * cw:(r + 1) * cw] = gg[r].reshape(cw)
    copies.append(pltpu.make_async_copy(flat, gg_out, sem.at[4]))
    copies[-1].start()
    for copy in copies:
        copy.wait()


def per_device(n, context, out_weight, cotangent, norm_gain, first_moment, second_moment):
    tok, heads = context.shape
    width = out_weight.shape[1]
    rows = first_moment.shape[1]
    bits = n.bit_length() - 1
    cw = 128
    quarter = width // (4 * cw)
    half, chunks = 2 * quarter, 4 * quarter
    stages = bits - 2
    cfg = (n, bits, quarter, cw, rows, tok, heads, width)
    sizes = [(n >> (s + 2)) * rows for s in range(stages)]
    dma = pltpu.SemaphoreType.DMA
    vmem = pltpu.VMEM
    scratch = [
        vmem((chunks, heads, cw), BF16),
        vmem((4 * tok, heads), BF16),
        vmem((n, rows, 2 * tok), F32),
        vmem((2, heads // 2, 2 * tok), BF16),
        vmem((half, tok, cw), BF16),
        vmem((width,), F32),
        vmem((chunks, 1, cw), F32),
        vmem((half, tok, cw), BF16),
        vmem((half, tok, cw), BF16),
        vmem((half, tok, cw), F32),
        vmem((8, tok), F32),
        vmem((8, tok), F32),
        vmem((tok, cw), F32),
        vmem((tok, cw), F32),
        vmem((half, 4 * tok, cw), BF16),
        vmem((half, tok, cw), BF16),
        tuple(vmem((half + 1, size, cw), BF16) for size in sizes),
        tuple(vmem((half + 1, size, cw), BF16) for size in sizes),
        tuple(vmem((half + 1, size, cw), F32) for size in sizes),
        vmem((half + 1, rows, cw), BF16),
        vmem((half + 1, rows, cw), BF16),
        vmem((2, rows, cw), F32),
        vmem((rows, width), F32),
        vmem((rows, width), F32),
        vmem((rows, width), BF16),
        vmem((tok, heads), F32),
        vmem((bits + 1, half, 1, cw), F32),
        vmem((bits + 1, half, 1, cw), F32),
        dma((2,)), dma((3,)), dma, dma((3,)),
        dma, dma((half,)), dma, dma, dma, dma((3,)),
        dma((2,)), dma, dma((half,)), dma((2,)), dma((half,)),
        dma((stages,)), dma((stages, half + 1)), dma, dma((half + 1,)),
        dma, dma((bits + 1,)),
    ]
    anywhere = pl.BlockSpec(memory_space=pltpu.HBM)
    pin = functools.partial(pltpu.with_memory_space_constraint, memory_space=pltpu.HBM)
    new_weight, new_first, new_second, grad_gain, grad_context = pl.pallas_call(
        functools.partial(kernel, cfg),
        out_shape=(
            jax.ShapeDtypeStruct(first_moment.shape, BF16),
            jax.ShapeDtypeStruct(first_moment.shape, F32),
            jax.ShapeDtypeStruct(first_moment.shape, F32),
            jax.ShapeDtypeStruct((chunks, 1, cw), F32),
            jax.ShapeDtypeStruct((tok, heads), BF16),
        ),
        in_specs=[anywhere] * 6,
        out_specs=(pl.BlockSpec(memory_space=pltpu.VMEM),) * 5,
        scratch_shapes=scratch,
        compiler_params=pltpu.CompilerParams(
            collective_id=0, has_side_effects=True, vmem_limit_bytes=VMEM_LIMIT
        ),
    )(*map(pin, (context, out_weight, cotangent, norm_gain, first_moment, second_moment)))
    return pl.pallas_call(
        settle,
        out_shape=(
            jax.ShapeDtypeStruct(first_moment.shape, BF16),
            jax.ShapeDtypeStruct(first_moment.shape, F32),
            jax.ShapeDtypeStruct(first_moment.shape, F32),
            jax.ShapeDtypeStruct((width,), F32),
            jax.ShapeDtypeStruct((tok, heads), BF16),
        ),
        in_specs=[pl.BlockSpec(memory_space=pltpu.VMEM)] * 5,
        out_specs=(anywhere,) * 5,
        scratch_shapes=[vmem((width,), F32), dma((5,))],
        compiler_params=pltpu.CompilerParams(vmem_limit_bytes=8 * 1024 * 1024),
    )(new_weight, new_first, new_second, grad_gain, grad_context)


def solution(mesh):
    return jax.shard_map(
        functools.partial(per_device, mesh.shape["dp"]),
        mesh=mesh,
        in_specs=(
            P("dp", "mp"),
            P("mp", None),
            P("dp", None),
            P(),
            P("mp", "dp", None),
            P("mp", "dp", None),
        ),
        out_specs=(
            P("mp", "dp", None),
            P("mp", "dp", None),
            P("mp", "dp", None),
            P(),
            P("dp", "mp"),
        ),
        check_vma=False,
    )
```

```python
import functools

import jax
import jax.numpy as jnp
from jax import lax
from jax.experimental import pallas as pl
from jax.experimental.pallas import tpu as pltpu
from jax.sharding import PartitionSpec as P

norm_floor = 0.1
learn_rate = 0.01
beta_one = 0.9
beta_two = 0.95
adam_floor = 1e-08

MESH = pl.DeviceIdType.MESH
F32 = jnp.float32
BF16 = jnp.bfloat16
VMEM_LIMIT = 50 * 1024 * 1024
LAG = 3
SWAP = 6
FIRST = 2
WARM = 3
MERGE = 4
MIX = 3


def kernel(
    cfg,
    ctx_hbm, w_hbm, cot_hbm, gain_hbm, m1_hbm, m2_hbm,
    nw, n1, n2, gfin, gc_out,
    wv, ctx, ctxt_all, ctxt, cot, gain_flat, gain, psend, precv, own, stat_s, stat_r, inverse_v, shift_v, g4, gx,
    sends, recvs, keeps, fsend, frecv, fkeep, m1, m2, master, gc_acc,
    gp, gpr,
    in_sem, w_sem, cot_sem, m_sem,
    ps_s, ps_r, st_s, st_r, cx_s, cx_r, gy_s, gx_s, gx_r, gm_s, gm_r,
    rs_s, rs_r, fx_s, fx_r, gg_s, gg_r,
):
    n, bits, quarter, cw, rows, tok, heads, width = cfg
    half = 2 * quarter
    chunks = 4 * quarter
    stages = bits - 2
    merged = half + 1 - MERGE
    dp, mp = lax.axis_index("dp"), lax.axis_index("mp")
    peer = 1 - mp
    side = (dp // 2) % 2
    order = [*range(2, bits), 1]

    def flip(index, bit):
        return index + (1 << bit) * (1 - 2 * ((index // (1 << bit)) % 2))

    def peer_id():
        return (dp, peer)

    def bit_id(bit):
        return (flip(dp, bit), mp)

    starts = [
        (2 * y_half + x_side) * quarter
        for x_side in (side, 1 - side) for y_half in (mp, peer)
    ]

    def cols(group, j):
        return pl.ds(pl.multiple_of((starts[group] + j) * cw, cw), cw)

    def cols_of(across, i):
        near, far = starts[2 * across:2 * across + 2]
        first = jnp.where(i < quarter, near + i, far + i - quarter)
        return pl.ds(pl.multiple_of(first * cw, cw), cw)

    def ctx_copy():
        return pltpu.make_async_copy(ctx_hbm, ctx.at[pl.ds(0, tok)], in_sem.at[0])

    def gain_copy():
        return pltpu.make_async_copy(gain_hbm, gain_flat, in_sem.at[1])

    def w_copy(group, j, sem):
        base = half * (1 - group % 2)
        return pltpu.make_async_copy(
            w_hbm.at[:, cols(group, j)], wv.at[base + 2 * j + group // 2], sem
        )

    def w_wait(first, last, sem):
        block = wv.at[pl.ds(first, last - first)]
        pltpu.make_async_copy(block, block, sem).wait()

    def cot_copy(far, j):
        h = far * quarter + j
        return pltpu.make_async_copy(cot_hbm.at[:, cols(2 * far, j)], cot.at[h], cot_sem)

    def m_copies():
        return (
            pltpu.make_async_copy(m1_hbm.at[0], m1, m_sem.at[0]),
            pltpu.make_async_copy(m2_hbm.at[0], m2, m_sem.at[1]),
            pltpu.make_async_copy(
                w_hbm.at[pl.ds(pl.multiple_of(dp * rows, rows), rows), :], master, m_sem.at[2]
            ),
        )

    def remote(src, dst, send_sem, recv_sem, device):
        return pltpu.make_async_remote_copy(
            src_ref=src, dst_ref=dst, send_sem=send_sem, recv_sem=recv_sem,
            device_id=device, device_id_type=MESH,
        )

    def partial_send(h):
        return remote(psend.at[h], precv.at[h], ps_s, ps_r.at[h], peer_id())

    def stat_send():
        return remote(stat_s, stat_r, st_s, st_r, peer_id())

    def ctx_send(a, b, i, bit):
        return remote(
            ctx.at[pl.ds(a * tok, tok)], ctx.at[pl.ds(b * tok, tok)], cx_s, cx_r.at[i], bit_id(bit)
        )

    def ctx_mate():
        return ctx_send(0, 1, 0, 0)

    def ctx_side():
        return ctx_send(0, 2, 1, 1)

    def ctx_relay():
        return ctx_send(2, 3, 2, 0)

    def grad_peer_near(j):
        return remote(
            g4.at[j, pl.ds(0, tok)], g4.at[quarter + j, pl.ds(0, tok)],
            gy_s.at[0], ps_r.at[j], peer_id(),
        )

    def grad_peer_far(j):
        return remote(
            gx.at[j], gx.at[quarter + j], gy_s.at[1], ps_r.at[quarter + j], peer_id()
        )

    def grad_side(i):
        return remote(gx.at[i], g4.at[i, pl.ds(2 * tok, tok)], gx_s, gx_r.at[i], bit_id(1))

    def grad_mate(i):
        return remote(
            g4.at[i, pl.ds(0, tok)], g4.at[i, pl.ds(tok, tok)], gm_s.at[0], gm_r.at[i], bit_id(0)
        )

    def grad_relay(i):
        return remote(
            g4.at[i, pl.ds(2 * tok, tok)], g4.at[i, pl.ds(3 * tok, tok)],
            gm_s.at[1], gm_r.at[i], bit_id(0),
        )

    def grad_chip(i):
        both = g4.at[i, pl.ds(0, 2 * tok)]
        return remote(both, both, gm_s.at[0], gm_r.at[i], bit_id(0))

    def shard_send(s, i):
        return remote(
            sends[s].at[i], recvs[s].at[i], rs_s.at[s], rs_r.at[s, i], bit_id(order[s])
        )

    def last_send(i, across):
        part = pl.ds(rows * (1 - across), rows)
        device = flip(dp, order[stages - 1])
        return remote(
            sends[-1].at[i, part], recvs[-1].at[i, part], rs_s.at[stages - 1], rs_r.at[stages - 1, i],
            (flip(device, 1) if across else device, mp),
        )

    def swap_send(i):
        other = jnp.where(i < 2, 1 - i, i)
        return remote(fsend.at[i], frecv.at[other], fx_s, fx_r.at[other], bit_id(1))

    def swap_wait(i):
        remote(fsend.at[i], frecv.at[i], fx_s, fx_r.at[i], bit_id(1)).wait_recv()

    steps = [0, *order]

    def gain_send(b):
        device = bit_id(steps[b]) if b < bits else peer_id()
        return remote(gp.at[b], gpr.at[b], gg_s, gg_r.at[b], device)

    barrier = pltpu.get_barrier_semaphore()
    pl.semaphore_signal(barrier, inc=1, device_id=peer_id(), device_id_type=MESH)
    for bit in range(bits - 1, -1, -1):
        pl.semaphore_signal(barrier, inc=1, device_id=bit_id(bit), device_id_type=MESH)

    diagonal = (flip(flip(dp, order[stages - 1]), 1), mp)
    pl.semaphore_signal(barrier, inc=1, device_id=diagonal, device_id_type=MESH)

    ctx_copy().start()
    w_copy(1, 0, w_sem.at[0]).start()
    w_copy(3, 0, w_sem.at[3]).start()

    def pair(base, j):
        right = jnp.concatenate([wv[base + 2 * j], wv[base + 2 * j + 1]], axis=1)
        return jnp.dot(ctx[0:tok], right, preferred_element_type=F32)

    def partial(j):
        value = pair(0, j).astype(BF16)
        psend[j] = value[:, :cw]
        psend[quarter + j] = value[:, cw:]

    def partial_start(j):
        partial_send(j).start()
        partial_send(quarter + j).start()

    ctx_copy().wait()
    w_wait(0, 1, w_sem.at[0])

    def partial_first(far):
        value = jnp.dot(ctx[0:tok], wv[far], preferred_element_type=F32)
        psend[far * quarter] = value.astype(BF16)

    partial_first(0)
    pl.semaphore_wait(barrier, bits + 2)

    partial_send(0).start()

    @pl.loop(1, quarter)
    def _(j):
        w_copy(1, j, w_sem.at[1]).start()
        w_copy(3, j, w_sem.at[1]).start()

    w_wait(1, 2, w_sem.at[3])
    partial_first(1)
    partial_send(quarter).start()

    @pl.loop(0, quarter)
    def _(j):
        w_copy(0, j, w_sem.at[2]).start()
        w_copy(2, j, w_sem.at[2]).start()

    w_wait(2, half, w_sem.at[1])

    @pl.loop(1, quarter)
    def _(j):
        partial(j)
        partial_start(j)
        cot_copy(0, j).start()
        cot_copy(1, j).start()

    ctx_side().start()
    ctx_mate().start()
    cot_copy(0, 0).start()
    cot_copy(1, 0).start()
    gain_copy().start()
    w_wait(half, chunks, w_sem.at[2])

    @pl.loop(0, quarter)
    def _(j):
        value = pair(half, j)
        own[j] = value[:, :cw]
        own[quarter + j] = value[:, cw:]

    for copy in m_copies():
        copy.start()

    gain_copy().wait()
    for r in range(chunks):
        gain[r] = gain_flat[r * cw:(r + 1) * cw].reshape(1, cw)

    def turn(p):
        ctxt_all[...] = jnp.transpose(
            ctx[2 * p * tok:2 * (p + 1) * tok].astype(F32)
        ).reshape(n, rows, 2 * tok)
        blocks = []
        for spot in range(n // 2):
            shard = dp
            for i, k in enumerate(order):
                if not (spot >> (bits - 2 - i)) & 1:
                    shard = flip(shard, k)
            blocks.append(ctxt_all[shard])
        ctxt[p] = jnp.concatenate(blocks, axis=0).astype(BF16)

    pltpu.make_async_copy(cot, cot, cot_sem).wait()
    ctx_mate().wait_recv()
    turn(0)

    def gather_stats(far, j, carry):
        square, cross = carry
        h = far * quarter + j
        partial_send(h).wait_recv()
        attn = own[h] + precv[h].astype(F32)
        own[h] = attn
        scaled = cot[h].astype(F32) * gain[starts[2 * far] + j]
        return square + attn * attn, cross + scaled * attn

    def gather_pair(j, carry):
        return gather_stats(1, j, gather_stats(0, j, carry))

    early, late = (2 * quarter) // 3, (5 * quarter) // 6
    zero = jnp.zeros((tok, cw), F32)
    carry = lax.fori_loop(0, early, gather_pair, (zero, zero))
    ctx_side().wait_recv()
    ctx_relay().start()
    carry = lax.fori_loop(early, late, gather_pair, carry)
    ctx_relay().wait_recv()
    turn(1)
    square, cross = lax.fori_loop(late, quarter, gather_pair, carry)
    square = jnp.sum(square, axis=1, keepdims=True)
    cross = jnp.sum(cross, axis=1, keepdims=True)
    even = lax.broadcasted_iota(jnp.int32, (tok, 128), 1) % 2 == 0
    stat_s[...] = jnp.transpose(jnp.where(even, square, cross))[0:8]
    stat_send().start()
    stat_send().wait_recv()
    totals = stat_s[...] + stat_r[...]

    def spread(row):
        return jnp.transpose(jnp.concatenate([totals[row:row + 1]] * 128, axis=0))

    inverse = lax.rsqrt(spread(0) / width + norm_floor)
    inverse_v[...] = inverse
    shift_v[...] = inverse * spread(1) / width

    def gradient(far, j):
        h = far * quarter + j
        spot = starts[2 * far] + j
        inverse = inverse_v[...]
        upstream = cot[h].astype(F32)
        normed = own[h] * inverse
        gp[0, spot - half * mp] = jnp.sum(upstream * normed, axis=0, keepdims=True)
        return (inverse * (upstream * gain[spot] - normed * shift_v[...])).astype(BF16)

    gx[0] = gradient(1, 0)
    g4[0, 2 * tok:3 * tok] = gx[0]
    grad_relay(0).start()
    grad_peer_far(0).start()
    g4[0, 0:tok] = gradient(0, 0)
    grad_mate(0).start()

    def far_part(j):
        gx[j] = gradient(1, j)
        grad_side(j).start()
        grad_peer_far(j).start()

    @pl.loop(1, FIRST)
    def _(j):
        far_part(j)

    def split(slot, product):
        cut = product.shape[0] // 2
        sends[0][slot] = product[:cut].astype(BF16)
        shard_send(0, slot).start()
        keeps[0][slot] = product[cut:]

    def first_products():
        grad_chip(0).wait_recv()
        for slot in range(2):
            split(slot, jnp.dot(
                ctxt[0], g4[0, 2 * slot * tok:2 * (slot + 1) * tok], preferred_element_type=F32
            ))

    @pl.when(dp % 2 == 0)
    def _():
        first_products()

    @pl.loop(1, quarter)
    def _(j):
        g4[j, 0:tok] = gradient(0, j)
        grad_mate(j).start()

    def context_part(u, base):
        left = jnp.concatenate([g4[u, 0:tok], gx[u]], axis=1)
        right = jnp.concatenate([wv[base], wv[base + 1]], axis=1)
        return lax.dot_general(left, right, (((1,), (1,)), ((), ())), preferred_element_type=F32)

    gc_acc[...] = context_part(0, half)

    @pl.loop(FIRST, quarter)
    def _(j):
        far_part(j)

        @pl.when(j >= quarter - MIX)
        def _():
            grad_peer_near(j - (quarter - MIX)).start()

    gain_send(0).start()

    @pl.loop(MIX, quarter)
    def _(j):
        grad_peer_near(j).start()

    def context_add(u):
        gc_acc[...] += context_part(u, half + 2 * u)

    warm = 1 + (WARM - 1) * (dp % 2)

    @pl.loop(1, warm)
    def _(u):
        context_add(u)

    @pl.when(dp % 2 == 1)
    def _():
        first_products()

    @pl.loop(warm, quarter)
    def _(u):
        context_add(u)

    def adam(total, cols):
        first = beta_one * m1[:, cols] + (1.0 - beta_one) * total
        second = beta_two * m2[:, cols] + (1.0 - beta_two) * total * total
        nw[0, :, cols] = (
            master[:, cols].astype(F32) - learn_rate * first / (jnp.sqrt(second) + adam_floor)
        ).astype(BF16)
        n1[0, :, cols] = first
        n2[0, :, cols] = second

    for copy in m_copies():
        copy.wait()

    swap_lag = LAG * stages + SWAP

    @pl.loop(1, max(half + swap_lag, 3 * bits + 6))
    def _(t):
        @pl.when(t < half)
        def _():
            grad_side(t).wait_recv()
            grad_relay(t).start()

        @pl.when((t >= quarter) & (t < half))
        def _():
            grad_peer_near(t - quarter).wait_recv()
            grad_mate(t).start()
            gc_acc[...] += context_part(t, 2 * (t - quarter))

        @pl.when(t == half)
        def _():
            gc_out[...] = gc_acc[...].astype(BF16)

        for b in range(bits + 1):
            @pl.when(t == 3 * b + 1 + 3 * (b >= bits - 1) + (b == bits))
            def _():
                gain_send(b).wait_recv()
                if b < bits:
                    gp[b + 1] = gp[b] + gpr[b]
                    gain_send(b + 1).start()
                else:
                    gfin[pl.ds(mp * half, half)] = gp[bits]
                    gfin[pl.ds(peer * half, half)] = gpr[bits]

        late_swap = t + 1 - swap_lag

        @pl.when((late_swap >= 0) & (late_swap <= half))
        def _():
            swap_wait(late_swap)
            total = frecv[late_swap].astype(F32)

            @pl.when(late_swap < 2)
            def _():
                first = jnp.where(late_swap == 0, starts[0], starts[2])
                adam(total + fkeep[late_swap], pl.ds(pl.multiple_of(first * cw, cw), cw))

            @pl.when((late_swap >= 2) & (late_swap < merged))
            def _():
                adam(total, cols_of(1, late_swap - 1))

            @pl.when(late_swap >= merged)
            def _():
                adam(total + recvs[-1][late_swap, 0:rows].astype(F32), cols_of(1, late_swap - 1))

        for s in range(stages - 1, -1, -1):
            i = t + 1 - LAG * (s + 1)

            @pl.when((i >= 0) & (i <= half))
            def _():
                shard_send(s, i).wait_recv()
                total = keeps[s][i] + recvs[s][i].astype(F32)
                cut = total.shape[0] // 2
                if s < stages - 1:
                    sends[s + 1][i] = total[:cut].astype(BF16)
                    if s < stages - 2:
                        shard_send(s + 1, i).start()
                    else:
                        @pl.when(i < merged)
                        def _():
                            shard_send(s + 1, i).start()

                        @pl.when(i >= merged)
                        def _():
                            last_send(i, 1).start()
                            last_send(i, 0).start()
                            fsend[i] = total[cut:cut + rows].astype(BF16)
                            swap_send(i).start()

                    keeps[s + 1][i] = total[cut:]
                else:
                    @pl.when(i < merged)
                    def _():
                        fsend[i] = total[:cut].astype(BF16)
                        swap_send(i).start()

                    @pl.when(i < 2)
                    def _():
                        fkeep[i] = total[cut:]

                    @pl.when(i >= 2)
                    def _():
                        adam(total[cut:], cols_of(0, i - 1))

        @pl.when(t < half)
        def _():
            grad_chip(t).wait_recv()
            product = jnp.dot(ctxt[0], g4[t, 0:2 * tok], preferred_element_type=F32)
            product += jnp.dot(ctxt[1], g4[t, 2 * tok:4 * tok], preferred_element_type=F32)
            split(t + 1, product)

        @pl.when(t <= quarter)
        def _():
            grad_peer_far(t - 1).wait_recv()
            grad_side(quarter + t - 1).start()

    def drain(block, sem):
        remote(block, block, sem, st_r, peer_id()).wait_send()

    stat_send().wait_send()
    drain(ctx.at[pl.ds(0, 3 * tok)], cx_s)
    drain(psend, ps_s)
    drain(gx.at[pl.ds(0, quarter)], gy_s.at[0])
    drain(gx.at[pl.ds(0, quarter)], gy_s.at[1])
    drain(gx.at[pl.ds(0, half - 1)], gx_s)
    drain(gx, gm_s.at[0])
    drain(gx, gm_s.at[1])
    drain(gp, gg_s)
    drain(fsend, fx_s)
    for s in range(stages):
        drain(sends[s], rs_s.at[s])


def settle(nw, n1, n2, gg, gc, nw_out, n1_out, n2_out, gg_out, gc_out, flat, sem):
    pairs = ((nw, nw_out), (n1, n1_out), (n2, n2_out), (gc, gc_out))
    copies = [pltpu.make_async_copy(a, b, sem.at[i]) for i, (a, b) in enumerate(pairs)]
    for copy in copies:
        copy.start()
    chunks, _, cw = gg.shape
    for r in range(chunks):
        flat[r * cw:(r + 1) * cw] = gg[r].reshape(cw)
    copies.append(pltpu.make_async_copy(flat, gg_out, sem.at[4]))
    copies[-1].start()
    for copy in copies:
        copy.wait()


def per_device(n, context, out_weight, cotangent, norm_gain, first_moment, second_moment):
    tok, heads = context.shape
    width = out_weight.shape[1]
    rows = first_moment.shape[1]
    bits = n.bit_length() - 1
    cw = 128
    quarter = width // (4 * cw)
    half, chunks = 2 * quarter, 4 * quarter
    stages = bits - 2
    cfg = (n, bits, quarter, cw, rows, tok, heads, width)
    sizes = [(n >> (s + 2)) * rows for s in range(stages)]
    dma = pltpu.SemaphoreType.DMA
    vmem = pltpu.VMEM
    scratch = [
        vmem((chunks, heads, cw), BF16),
        vmem((4 * tok, heads), BF16),
        vmem((n, rows, 2 * tok), F32),
        vmem((2, heads // 2, 2 * tok), BF16),
        vmem((half, tok, cw), BF16),
        vmem((width,), F32),
        vmem((chunks, 1, cw), F32),
        vmem((half, tok, cw), BF16),
        vmem((half, tok, cw), BF16),
        vmem((half, tok, cw), F32),
        vmem((8, tok), F32),
        vmem((8, tok), F32),
        vmem((tok, cw), F32),
        vmem((tok, cw), F32),
        vmem((half, 4 * tok, cw), BF16),
        vmem((half, tok, cw), BF16),
        tuple(vmem((half + 1, size, cw), BF16) for size in sizes),
        tuple(vmem((half + 1, size, cw), BF16) for size in sizes),
        tuple(vmem((half + 1, size, cw), F32) for size in sizes),
        vmem((half + 1, rows, cw), BF16),
        vmem((half + 1, rows, cw), BF16),
        vmem((2, rows, cw), F32),
        vmem((rows, width), F32),
        vmem((rows, width), F32),
        vmem((rows, width), BF16),
        vmem((tok, heads), F32),
        vmem((bits + 1, half, 1, cw), F32),
        vmem((bits + 1, half, 1, cw), F32),
        dma((2,)), dma((4,)), dma, dma((3,)),
        dma, dma((half,)), dma, dma, dma, dma((3,)),
        dma((2,)), dma, dma((half,)), dma((2,)), dma((half,)),
        dma((stages,)), dma((stages, half + 1)), dma, dma((half + 1,)),
        dma, dma((bits + 1,)),
    ]
    anywhere = pl.BlockSpec(memory_space=pltpu.HBM)
    pin = functools.partial(pltpu.with_memory_space_constraint, memory_space=pltpu.HBM)
    new_weight, new_first, new_second, grad_gain, grad_context = pl.pallas_call(
        functools.partial(kernel, cfg),
        out_shape=(
            jax.ShapeDtypeStruct(first_moment.shape, BF16),
            jax.ShapeDtypeStruct(first_moment.shape, F32),
            jax.ShapeDtypeStruct(first_moment.shape, F32),
            jax.ShapeDtypeStruct((chunks, 1, cw), F32),
            jax.ShapeDtypeStruct((tok, heads), BF16),
        ),
        in_specs=[anywhere] * 6,
        out_specs=(pl.BlockSpec(memory_space=pltpu.VMEM),) * 5,
        scratch_shapes=scratch,
        compiler_params=pltpu.CompilerParams(
            collective_id=0, has_side_effects=True, vmem_limit_bytes=VMEM_LIMIT
        ),
    )(*map(pin, (context, out_weight, cotangent, norm_gain, first_moment, second_moment)))
    return pl.pallas_call(
        settle,
        out_shape=(
            jax.ShapeDtypeStruct(first_moment.shape, BF16),
            jax.ShapeDtypeStruct(first_moment.shape, F32),
            jax.ShapeDtypeStruct(first_moment.shape, F32),
            jax.ShapeDtypeStruct((width,), F32),
            jax.ShapeDtypeStruct((tok, heads), BF16),
        ),
        in_specs=[pl.BlockSpec(memory_space=pltpu.VMEM)] * 5,
        out_specs=(anywhere,) * 5,
        scratch_shapes=[vmem((width,), F32), dma((5,))],
        compiler_params=pltpu.CompilerParams(vmem_limit_bytes=8 * 1024 * 1024),
    )(new_weight, new_first, new_second, grad_gain, grad_context)


def solution(mesh):
    return jax.shard_map(
        functools.partial(per_device, mesh.shape["dp"]),
        mesh=mesh,
        in_specs=(
            P("dp", "mp"),
            P("mp", None),
            P("dp", None),
            P(),
            P("mp", "dp", None),
            P("mp", "dp", None),
        ),
        out_specs=(
            P("mp", "dp", None),
            P("mp", "dp", None),
            P("mp", "dp", None),
            P(),
            P("dp", "mp"),
        ),
        check_vma=False,
    )
```

```python
import functools

import jax
import jax.numpy as jnp
from jax import lax
from jax.experimental import pallas as pl
from jax.experimental.pallas import tpu as pltpu
from jax.sharding import PartitionSpec as P

norm_floor = 0.1
learn_rate = 0.01
beta_one = 0.9
beta_two = 0.95
adam_floor = 1e-08

MESH = pl.DeviceIdType.MESH
F32 = jnp.float32
BF16 = jnp.bfloat16
VMEM_LIMIT = 50 * 1024 * 1024
LAG = 3
SWAP = 6
FIRST = 2
WARM = 3
MERGE = 4
MIX = 3


def kernel(
    cfg,
    ctx_hbm, w_hbm, cot_hbm, gain_hbm, m1_hbm, m2_hbm,
    nw, n1, n2, gfin, gc_out,
    wv, ctx, ctxt_all, ctxt, cot, gain_flat, gain, psend, precv, own, stat_s, stat_r, inverse_v, shift_v, g4, gx,
    sends, recvs, keeps, fsend, frecv, fkeep, m1, m2, master, gc_acc,
    gp, gpr,
    in_sem, w_sem, cot_sem, m_sem,
    ps_s, ps_r, st_s, st_r, cx_s, cx_r, gy_s, gx_s, gx_r, gm_s, gm_r,
    rs_s, rs_r, fx_s, fx_r, gg_s, gg_r,
):
    n, bits, quarter, cw, rows, tok, heads, width = cfg
    half = 2 * quarter
    chunks = 4 * quarter
    stages = bits - 2
    merged = half + 1 - MERGE
    dp, mp = lax.axis_index("dp"), lax.axis_index("mp")
    peer = 1 - mp
    side = (dp // 2) % 2
    order = [*range(2, bits), 1]

    def flip(index, bit):
        return index + (1 << bit) * (1 - 2 * ((index // (1 << bit)) % 2))

    def peer_id():
        return (dp, peer)

    def bit_id(bit):
        return (flip(dp, bit), mp)

    starts = [
        (2 * y_half + x_side) * quarter
        for x_side in (side, 1 - side) for y_half in (mp, peer)
    ]

    def cols(group, j):
        return pl.ds(pl.multiple_of((starts[group] + j) * cw, cw), cw)

    def cols_of(across, i):
        near, far = starts[2 * across:2 * across + 2]
        first = jnp.where(i < quarter, near + i, far + i - quarter)
        return pl.ds(pl.multiple_of(first * cw, cw), cw)

    def ctx_copy():
        return pltpu.make_async_copy(ctx_hbm, ctx.at[pl.ds(0, tok)], in_sem.at[0])

    def gain_copy():
        return pltpu.make_async_copy(gain_hbm, gain_flat, in_sem.at[1])

    def w_copy(group, j, sem):
        base = half * (1 - group % 2)
        return pltpu.make_async_copy(
            w_hbm.at[:, cols(group, j)], wv.at[base + 2 * j + group // 2], sem
        )

    def w_wait(first, last, sem):
        block = wv.at[pl.ds(first, last - first)]
        pltpu.make_async_copy(block, block, sem).wait()

    def cot_copy(far, j):
        h = far * quarter + j
        return pltpu.make_async_copy(cot_hbm.at[:, cols(2 * far, j)], cot.at[h], cot_sem)

    def m_copies():
        return (
            pltpu.make_async_copy(m1_hbm.at[0], m1, m_sem.at[0]),
            pltpu.make_async_copy(m2_hbm.at[0], m2, m_sem.at[1]),
            pltpu.make_async_copy(
                w_hbm.at[pl.ds(pl.multiple_of(dp * rows, rows), rows), :], master, m_sem.at[2]
            ),
        )

    def remote(src, dst, send_sem, recv_sem, device):
        return pltpu.make_async_remote_copy(
            src_ref=src, dst_ref=dst, send_sem=send_sem, recv_sem=recv_sem,
            device_id=device, device_id_type=MESH,
        )

    def partial_send(h):
        return remote(psend.at[h], precv.at[h], ps_s, ps_r.at[h], peer_id())

    def stat_send():
        return remote(stat_s, stat_r, st_s, st_r, peer_id())

    def ctx_send(a, b, i, bit):
        return remote(
            ctx.at[pl.ds(a * tok, tok)], ctx.at[pl.ds(b * tok, tok)], cx_s, cx_r.at[i], bit_id(bit)
        )

    def ctx_mate():
        return ctx_send(0, 1, 0, 0)

    def ctx_side():
        return ctx_send(0, 2, 1, 1)

    def ctx_relay():
        return ctx_send(2, 3, 2, 0)

    def grad_peer_near(j):
        return remote(
            g4.at[j, pl.ds(0, tok)], g4.at[quarter + j, pl.ds(0, tok)],
            gy_s.at[0], ps_r.at[j], peer_id(),
        )

    def grad_peer_far(j):
        return remote(
            gx.at[j], gx.at[quarter + j], gy_s.at[1], ps_r.at[quarter + j], peer_id()
        )

    def grad_side(i):
        return remote(gx.at[i], g4.at[i, pl.ds(2 * tok, tok)], gx_s, gx_r.at[i], bit_id(1))

    def grad_mate(i):
        return remote(
            g4.at[i, pl.ds(0, tok)], g4.at[i, pl.ds(tok, tok)], gm_s.at[0], gm_r.at[i], bit_id(0)
        )

    def grad_relay(i):
        return remote(
            g4.at[i, pl.ds(2 * tok, tok)], g4.at[i, pl.ds(3 * tok, tok)],
            gm_s.at[1], gm_r.at[i], bit_id(0),
        )

    def grad_chip(i):
        both = g4.at[i, pl.ds(0, 2 * tok)]
        return remote(both, both, gm_s.at[0], gm_r.at[i], bit_id(0))

    def shard_send(s, i):
        return remote(
            sends[s].at[i], recvs[s].at[i], rs_s.at[s], rs_r.at[s, i], bit_id(order[s])
        )

    def last_send(i, across):
        part = pl.ds(rows * (1 - across), rows)
        device = flip(dp, order[stages - 1])
        return remote(
            sends[-1].at[i, part], recvs[-1].at[i, part], rs_s.at[stages - 1], rs_r.at[stages - 1, i],
            (flip(device, 1) if across else device, mp),
        )

    def swap_send(i):
        other = jnp.where(i < 2, 1 - i, i)
        return remote(fsend.at[i], frecv.at[other], fx_s, fx_r.at[other], bit_id(1))

    def swap_wait(i):
        remote(fsend.at[i], frecv.at[i], fx_s, fx_r.at[i], bit_id(1)).wait_recv()

    steps = [0, *order]

    def gain_send(b):
        device = bit_id(steps[b]) if b < bits else peer_id()
        return remote(gp.at[b], gpr.at[b], gg_s, gg_r.at[b], device)

    barrier = pltpu.get_barrier_semaphore()
    pl.semaphore_signal(barrier, inc=1, device_id=peer_id(), device_id_type=MESH)
    for bit in range(bits - 1, -1, -1):
        pl.semaphore_signal(barrier, inc=1, device_id=bit_id(bit), device_id_type=MESH)

    diagonal = (flip(flip(dp, order[stages - 1]), 1), mp)
    pl.semaphore_signal(barrier, inc=1, device_id=diagonal, device_id_type=MESH)

    ctx_copy().start()
    w_copy(1, 0, w_sem.at[0]).start()
    w_copy(3, 0, w_sem.at[3]).start()

    def pair(base, j):
        right = jnp.concatenate([wv[base + 2 * j], wv[base + 2 * j + 1]], axis=1)
        return jnp.dot(ctx[0:tok], right, preferred_element_type=F32)

    def partial(j):
        value = pair(0, j).astype(BF16)
        psend[j] = value[:, :cw]
        psend[quarter + j] = value[:, cw:]

    def partial_start(j):
        partial_send(j).start()
        partial_send(quarter + j).start()

    ctx_copy().wait()
    w_wait(0, 1, w_sem.at[0])

    def partial_first(far):
        value = jnp.dot(ctx[0:tok], wv[far], preferred_element_type=F32)
        psend[far * quarter] = value.astype(BF16)

    partial_first(0)
    pl.semaphore_wait(barrier, bits + 2)

    partial_send(0).start()

    @pl.loop(1, quarter)
    def _(j):
        w_copy(1, j, w_sem.at[1]).start()
        w_copy(3, j, w_sem.at[1]).start()

    w_wait(1, 2, w_sem.at[3])
    partial_first(1)
    partial_send(quarter).start()

    @pl.loop(0, quarter)
    def _(j):
        w_copy(0, j, w_sem.at[2]).start()
        w_copy(2, j, w_sem.at[2]).start()

    w_wait(2, half, w_sem.at[1])

    @pl.loop(1, quarter)
    def _(j):
        partial(j)
        partial_start(j)
        cot_copy(0, j).start()
        cot_copy(1, j).start()

    ctx_side().start()
    ctx_mate().start()
    cot_copy(0, 0).start()
    cot_copy(1, 0).start()
    gain_copy().start()
    w_wait(half, chunks, w_sem.at[2])

    @pl.loop(0, quarter)
    def _(j):
        value = pair(half, j)
        own[j] = value[:, :cw]
        own[quarter + j] = value[:, cw:]

    for copy in m_copies():
        copy.start()

    gain_copy().wait()
    for r in range(chunks):
        gain[r] = gain_flat[r * cw:(r + 1) * cw].reshape(1, cw)

    def turn(p):
        ctxt_all[...] = jnp.transpose(
            ctx[2 * p * tok:2 * (p + 1) * tok].astype(F32)
        ).reshape(n, rows, 2 * tok)
        blocks = []
        for spot in range(n // 2):
            shard = dp
            for i, k in enumerate(order):
                if not (spot >> (bits - 2 - i)) & 1:
                    shard = flip(shard, k)
            blocks.append(ctxt_all[shard])
        ctxt[p] = jnp.concatenate(blocks, axis=0).astype(BF16)

    pltpu.make_async_copy(cot, cot, cot_sem).wait()
    ctx_mate().wait_recv()
    turn(0)

    def gather_stats(far, j, carry):
        square, cross = carry
        h = far * quarter + j
        partial_send(h).wait_recv()
        attn = own[h] + precv[h].astype(F32)
        own[h] = attn
        scaled = cot[h].astype(F32) * gain[starts[2 * far] + j]
        return square + attn * attn, cross + scaled * attn

    def gather_pair(j, carry):
        return gather_stats(1, j, gather_stats(0, j, carry))

    early, late = (2 * quarter) // 3, (5 * quarter) // 6
    zero = jnp.zeros((tok, cw), F32)
    carry = lax.fori_loop(0, early, gather_pair, (zero, zero))
    ctx_side().wait_recv()
    ctx_relay().start()
    carry = lax.fori_loop(early, late, gather_pair, carry)
    ctx_relay().wait_recv()
    turn(1)
    square, cross = lax.fori_loop(late, quarter, gather_pair, carry)
    square = jnp.sum(square, axis=1, keepdims=True)
    cross = jnp.sum(cross, axis=1, keepdims=True)
    even = lax.broadcasted_iota(jnp.int32, (tok, 128), 1) % 2 == 0
    stat_s[...] = jnp.transpose(jnp.where(even, square, cross))[0:2]
    stat_send().start()
    stat_send().wait_recv()
    totals = stat_s[...] + stat_r[...]

    def spread(row):
        return jnp.transpose(jnp.concatenate([totals[row:row + 1]] * 128, axis=0))

    inverse = lax.rsqrt(spread(0) / width + norm_floor)
    inverse_v[...] = inverse
    shift_v[...] = inverse * spread(1) / width

    def gradient(far, j):
        h = far * quarter + j
        spot = starts[2 * far] + j
        inverse = inverse_v[...]
        upstream = cot[h].astype(F32)
        normed = own[h] * inverse
        gp[0, spot - half * mp] = jnp.sum(upstream * normed, axis=0, keepdims=True)
        return (inverse * (upstream * gain[spot] - normed * shift_v[...])).astype(BF16)

    gx[0] = gradient(1, 0)
    g4[0, 2 * tok:3 * tok] = gx[0]
    grad_relay(0).start()
    grad_peer_far(0).start()
    g4[0, 0:tok] = gradient(0, 0)
    grad_mate(0).start()

    def far_part(j):
        gx[j] = gradient(1, j)
        grad_side(j).start()
        grad_peer_far(j).start()

    @pl.loop(1, FIRST)
    def _(j):
        far_part(j)

    def split(slot, product):
        cut = product.shape[0] // 2
        sends[0][slot] = product[:cut].astype(BF16)
        shard_send(0, slot).start()
        keeps[0][slot] = product[cut:]

    def first_products():
        grad_chip(0).wait_recv()
        for slot in range(2):
            split(slot, jnp.dot(
                ctxt[0], g4[0, 2 * slot * tok:2 * (slot + 1) * tok], preferred_element_type=F32
            ))

    @pl.when(dp % 2 == 0)
    def _():
        first_products()

    @pl.loop(1, quarter)
    def _(j):
        g4[j, 0:tok] = gradient(0, j)
        grad_mate(j).start()

    def context_part(u, base):
        left = jnp.concatenate([g4[u, 0:tok], gx[u]], axis=1)
        right = jnp.concatenate([wv[base], wv[base + 1]], axis=1)
        return lax.dot_general(left, right, (((1,), (1,)), ((), ())), preferred_element_type=F32)

    gc_acc[...] = context_part(0, half)

    @pl.loop(FIRST, quarter)
    def _(j):
        far_part(j)

        @pl.when(j >= quarter - MIX)
        def _():
            grad_peer_near(j - (quarter - MIX)).start()

    gain_send(0).start()

    @pl.loop(MIX, quarter)
    def _(j):
        grad_peer_near(j).start()

    def context_add(u):
        gc_acc[...] += context_part(u, half + 2 * u)

    warm = 1 + (WARM - 1) * (dp % 2)

    @pl.loop(1, warm)
    def _(u):
        context_add(u)

    @pl.when(dp % 2 == 1)
    def _():
        first_products()

    @pl.loop(warm, quarter)
    def _(u):
        context_add(u)

    def adam(total, cols):
        first = beta_one * m1[:, cols] + (1.0 - beta_one) * total
        second = beta_two * m2[:, cols] + (1.0 - beta_two) * total * total
        nw[0, :, cols] = (
            master[:, cols].astype(F32) - learn_rate * first / (jnp.sqrt(second) + adam_floor)
        ).astype(BF16)
        n1[0, :, cols] = first
        n2[0, :, cols] = second

    for copy in m_copies():
        copy.wait()

    swap_lag = LAG * stages + SWAP

    @pl.loop(1, max(half + swap_lag, 3 * bits + 6))
    def _(t):
        @pl.when(t < half)
        def _():
            grad_side(t).wait_recv()
            grad_relay(t).start()

        @pl.when((t >= quarter) & (t < half))
        def _():
            grad_peer_near(t - quarter).wait_recv()
            grad_mate(t).start()
            gc_acc[...] += context_part(t, 2 * (t - quarter))

        @pl.when(t == half)
        def _():
            gc_out[...] = gc_acc[...].astype(BF16)

        for b in range(bits + 1):
            @pl.when(t == 3 * b + 1 + 3 * (b >= bits - 1) + (b == bits))
            def _():
                gain_send(b).wait_recv()
                if b < bits:
                    gp[b + 1] = gp[b] + gpr[b]
                    gain_send(b + 1).start()
                else:
                    gfin[pl.ds(mp * half, half)] = gp[bits]
                    gfin[pl.ds(peer * half, half)] = gpr[bits]

        late_swap = t + 1 - swap_lag

        @pl.when((late_swap >= 0) & (late_swap <= half))
        def _():
            swap_wait(late_swap)
            total = frecv[late_swap].astype(F32)

            @pl.when(late_swap < 2)
            def _():
                first = jnp.where(late_swap == 0, starts[0], starts[2])
                adam(total + fkeep[late_swap], pl.ds(pl.multiple_of(first * cw, cw), cw))

            @pl.when((late_swap >= 2) & (late_swap < merged))
            def _():
                adam(total, cols_of(1, late_swap - 1))

            @pl.when(late_swap >= merged)
            def _():
                adam(total + recvs[-1][late_swap, 0:rows].astype(F32), cols_of(1, late_swap - 1))

        for s in range(stages - 1, -1, -1):
            i = t + 1 - LAG * (s + 1)

            @pl.when((i >= 0) & (i <= half))
            def _():
                shard_send(s, i).wait_recv()
                total = keeps[s][i] + recvs[s][i].astype(F32)
                cut = total.shape[0] // 2
                if s < stages - 1:
                    sends[s + 1][i] = total[:cut].astype(BF16)
                    if s < stages - 2:
                        shard_send(s + 1, i).start()
                    else:
                        @pl.when(i < merged)
                        def _():
                            shard_send(s + 1, i).start()

                        @pl.when(i >= merged)
                        def _():
                            last_send(i, 1).start()
                            last_send(i, 0).start()
                            fsend[i] = total[cut:cut + rows].astype(BF16)
                            swap_send(i).start()

                    keeps[s + 1][i] = total[cut:]
                else:
                    @pl.when(i < merged)
                    def _():
                        fsend[i] = total[:cut].astype(BF16)
                        swap_send(i).start()

                    @pl.when(i < 2)
                    def _():
                        fkeep[i] = total[cut:]

                    @pl.when(i >= 2)
                    def _():
                        adam(total[cut:], cols_of(0, i - 1))

        @pl.when(t < half)
        def _():
            grad_chip(t).wait_recv()
            product = jnp.dot(ctxt[0], g4[t, 0:2 * tok], preferred_element_type=F32)
            product += jnp.dot(ctxt[1], g4[t, 2 * tok:4 * tok], preferred_element_type=F32)
            split(t + 1, product)

        @pl.when(t <= quarter)
        def _():
            grad_peer_far(t - 1).wait_recv()
            grad_side(quarter + t - 1).start()

    def drain(block, sem):
        remote(block, block, sem, st_r, peer_id()).wait_send()

    stat_send().wait_send()
    drain(ctx.at[pl.ds(0, 3 * tok)], cx_s)
    drain(psend, ps_s)
    drain(gx.at[pl.ds(0, quarter)], gy_s.at[0])
    drain(gx.at[pl.ds(0, quarter)], gy_s.at[1])
    drain(gx.at[pl.ds(0, half - 1)], gx_s)
    drain(gx, gm_s.at[0])
    drain(gx, gm_s.at[1])
    drain(gp, gg_s)
    drain(fsend, fx_s)
    for s in range(stages):
        drain(sends[s], rs_s.at[s])


def settle(nw, n1, n2, gg, gc, nw_out, n1_out, n2_out, gg_out, gc_out, flat, sem):
    pairs = ((nw, nw_out), (n1, n1_out), (n2, n2_out), (gc, gc_out))
    copies = [pltpu.make_async_copy(a, b, sem.at[i]) for i, (a, b) in enumerate(pairs)]
    for copy in copies:
        copy.start()
    chunks, _, cw = gg.shape
    for r in range(chunks):
        flat[r * cw:(r + 1) * cw] = gg[r].reshape(cw)
    copies.append(pltpu.make_async_copy(flat, gg_out, sem.at[4]))
    copies[-1].start()
    for copy in copies:
        copy.wait()


def per_device(n, context, out_weight, cotangent, norm_gain, first_moment, second_moment):
    tok, heads = context.shape
    width = out_weight.shape[1]
    rows = first_moment.shape[1]
    bits = n.bit_length() - 1
    cw = 128
    quarter = width // (4 * cw)
    half, chunks = 2 * quarter, 4 * quarter
    stages = bits - 2
    cfg = (n, bits, quarter, cw, rows, tok, heads, width)
    sizes = [(n >> (s + 2)) * rows for s in range(stages)]
    dma = pltpu.SemaphoreType.DMA
    vmem = pltpu.VMEM
    scratch = [
        vmem((chunks, heads, cw), BF16),
        vmem((4 * tok, heads), BF16),
        vmem((n, rows, 2 * tok), F32),
        vmem((2, heads // 2, 2 * tok), BF16),
        vmem((half, tok, cw), BF16),
        vmem((width,), F32),
        vmem((chunks, 1, cw), F32),
        vmem((half, tok, cw), BF16),
        vmem((half, tok, cw), BF16),
        vmem((half, tok, cw), F32),
        vmem((2, tok), F32),
        vmem((2, tok), F32),
        vmem((tok, cw), F32),
        vmem((tok, cw), F32),
        vmem((half, 4 * tok, cw), BF16),
        vmem((half, tok, cw), BF16),
        tuple(vmem((half + 1, size, cw), BF16) for size in sizes),
        tuple(vmem((half + 1, size, cw), BF16) for size in sizes),
        tuple(vmem((half + 1, size, cw), F32) for size in sizes),
        vmem((half + 1, rows, cw), BF16),
        vmem((half + 1, rows, cw), BF16),
        vmem((2, rows, cw), F32),
        vmem((rows, width), F32),
        vmem((rows, width), F32),
        vmem((rows, width), BF16),
        vmem((tok, heads), F32),
        vmem((bits + 1, half, 1, cw), F32),
        vmem((bits + 1, half, 1, cw), F32),
        dma((2,)), dma((4,)), dma, dma((3,)),
        dma, dma((half,)), dma, dma, dma, dma((3,)),
        dma((2,)), dma, dma((half,)), dma((2,)), dma((half,)),
        dma((stages,)), dma((stages, half + 1)), dma, dma((half + 1,)),
        dma, dma((bits + 1,)),
    ]
    anywhere = pl.BlockSpec(memory_space=pltpu.HBM)
    pin = functools.partial(pltpu.with_memory_space_constraint, memory_space=pltpu.HBM)
    new_weight, new_first, new_second, grad_gain, grad_context = pl.pallas_call(
        functools.partial(kernel, cfg),
        out_shape=(
            jax.ShapeDtypeStruct(first_moment.shape, BF16),
            jax.ShapeDtypeStruct(first_moment.shape, F32),
            jax.ShapeDtypeStruct(first_moment.shape, F32),
            jax.ShapeDtypeStruct((chunks, 1, cw), F32),
            jax.ShapeDtypeStruct((tok, heads), BF16),
        ),
        in_specs=[anywhere] * 6,
        out_specs=(pl.BlockSpec(memory_space=pltpu.VMEM),) * 5,
        scratch_shapes=scratch,
        compiler_params=pltpu.CompilerParams(
            collective_id=0, has_side_effects=True, vmem_limit_bytes=VMEM_LIMIT
        ),
    )(*map(pin, (context, out_weight, cotangent, norm_gain, first_moment, second_moment)))
    return pl.pallas_call(
        settle,
        out_shape=(
            jax.ShapeDtypeStruct(first_moment.shape, BF16),
            jax.ShapeDtypeStruct(first_moment.shape, F32),
            jax.ShapeDtypeStruct(first_moment.shape, F32),
            jax.ShapeDtypeStruct((width,), F32),
            jax.ShapeDtypeStruct((tok, heads), BF16),
        ),
        in_specs=[pl.BlockSpec(memory_space=pltpu.VMEM)] * 5,
        out_specs=(anywhere,) * 5,
        scratch_shapes=[vmem((width,), F32), dma((5,))],
        compiler_params=pltpu.CompilerParams(vmem_limit_bytes=8 * 1024 * 1024),
    )(new_weight, new_first, new_second, grad_gain, grad_context)


def solution(mesh):
    return jax.shard_map(
        functools.partial(per_device, mesh.shape["dp"]),
        mesh=mesh,
        in_specs=(
            P("dp", "mp"),
            P("mp", None),
            P("dp", None),
            P(),
            P("mp", "dp", None),
            P("mp", "dp", None),
        ),
        out_specs=(
            P("mp", "dp", None),
            P("mp", "dp", None),
            P("mp", "dp", None),
            P(),
            P("dp", "mp"),
        ),
        check_vma=False,
    )
```
